512 devices in a mesh: row: 8 (over y), col: 16 (over z, core), rhs: 4 (over x).
Axes of the slice: x: 4, y: 8, z: 8, core: 2. Of those that a mesh axis runs over, the one named last changes fastest.
Arguments:
- points: bfloat16 [64, 786432], P(None, ('row', 'col')), may hold values from -6 to 6
- vectors: bfloat16 [64, 786432], P('rhs', ('row', 'col')), may hold values from -6 to 6
- leaf_basis: bfloat16 [1536, 512, 128], P(('row', 'col')), may hold values from -0.25 to 0.25
- leaf_transfer: bfloat16 [1536, 128, 128], P(('row', 'col')), may hold values from -0.375 to 0.375
- node_transfer: bfloat16 [128, 128, 128], P(('row', 'col')), may hold values from -0.375 to 0.375
- leaf_coupling: bfloat16 [1536, 3, 128, 128], P(('row', 'col')), may hold values from -0.3125 to 0.3125
- node_coupling: bfloat16 [128, 6, 128, 128], P(('row', 'col')), may hold values from -0.09375 to 0.09375
- top_coupling: bfloat16 [16, 16, 128, 128], P('col'), may hold values from -0.02734375 to 0.02734375
- near_list: int32 [1536, 5], P(('row', 'col')), may hold values from 0 to 1535, as said below
- near_count: int32 [1536], P(('row', 'col')), may hold values from 1 to 5, as said below
- far_leaves: int32 [1536, 3], P(('row', 'col')), may hold values from 0 to 1535, as said below
- far_nodes: int32 [128, 6], P(('row', 'col')), may hold values from 0 to 127, as said below
Outputs:
- product: bfloat16 [64, 786432], P('rhs', ('row', 'col'))
The draws below stay inside these ranges and needn't reach their ends.
Inputs may be any that keep to these rules, and one draw needn't show every extreme that they name: `near_list`: the first entry of row l is l itself; all entries of a row are distinct and lie in the window of leaves j with (j // 12 - l // 12) mod (128) in the finite set (-1, 0, 1), cyclically. Entries from near_count[l] on are not used. `near_count`: some leaf has 5 used entries. `far_leaves`: entries of a row are distinct, lie in the same cyclic window as the near rows, and differ from all 5 entries of the leaf's near row. `far_nodes`: entries of a row are distinct and never the node itself.
All inputs are finite; a program needn't handle non-finite values.
Results may differ from the reference program's by a relative error of at most 0.01.
Values may be sent and summed in bfloat16 or wider, within the bound.
A program may use at most 64 MiB of HBM per device.

```python
import jax
import jax.numpy as jnp
from jax import lax

FEAT = 64
LEAF = 512
RANK = 128
LEAF_DEV = 12
NEAR_MOST = 5
FARL = 3
FARB = 6
NB = 128
NLEAVES = 1536
NPTS = 786432
RHS = 64
N_ROW = 8
N_COL = 16


def window_lists(key):
    leaf_ids = jnp.arange(NLEAVES, dtype=jnp.int32)
    offsets = jnp.arange(3 * LEAF_DEV, dtype=jnp.int32)
    starts = (leaf_ids // LEAF_DEV - 1) * LEAF_DEV
    candidates = (starts[:, None] + offsets[None, :]) % NLEAVES
    own_slot = LEAF_DEV + leaf_ids % LEAF_DEV
    scores = jax.random.randint(jax.random.fold_in(key, 17), (NLEAVES, 3 * LEAF_DEV), 0, 1048576) * 128 + offsets[None, :]
    scores = jnp.where(offsets[None, :] == own_slot[:, None], -1, scores)
    ordering = jnp.argsort(scores, axis=1, stable=True)
    return jnp.take_along_axis(candidates, ordering, axis=1).astype(jnp.int32)


def draw_near_list(key, part):
    return window_lists(key)[:, :NEAR_MOST]


def draw_far_leaves(key, part):
    return window_lists(key)[:, NEAR_MOST:NEAR_MOST + FARL]


def draw_near_count(key, part):
    first_draw = jax.random.randint(jax.random.fold_in(key, 23), (NLEAVES,), 1, NEAR_MOST + 1)
    second_draw = jax.random.randint(jax.random.fold_in(key, 29), (NLEAVES,), 1, NEAR_MOST + 1)
    chosen = jax.random.randint(jax.random.fold_in(key, 31), (), 0, NLEAVES)
    counts = jnp.minimum(first_draw, second_draw)
    counts = jnp.where(jnp.arange(NLEAVES) == chosen, NEAR_MOST, counts)
    return counts.astype(jnp.int32)


def draw_far_nodes(key, part):
    node_ids = jnp.arange(NB, dtype=jnp.int32)
    scores = jax.random.randint(jax.random.fold_in(key, 37), (NB, NB), 0, 1048576) * 512 + node_ids[None, :]
    scores = jnp.where(node_ids[None, :] == node_ids[:, None], 1073741824, scores)
    ordering = jnp.argsort(scores, axis=1, stable=True)
    return ordering[:, :FARB].astype(jnp.int32)


def steps_of(key, dims, shards, low, high):
    def one(dim, shards_of):
        draws = jax.random.uniform(jax.random.fold_in(jax.random.fold_in(key, 6), dim), (shards_of,), jnp.float32, low / len(shards), high / len(shards))
        return jnp.repeat(jnp.exp(draws), dims[dim] // shards_of).reshape((-1,) + (1,) * (len(dims) - dim - 1))

    gain = one(*shards[0])
    for cut in shards[1:]:
        gain = gain * one(*cut)
    return gain


def bell_draw(rng, dims, deviation, bound, pieces=(), kind=jnp.bfloat16):
    values = jax.random.normal(rng, dims, jnp.float32) * deviation
    if len(pieces) > 0:
        values = steps_of(rng, dims, pieces, -0.22, 0.18) * values
    return jnp.clip(values, min=-bound, max=bound).astype(kind)


def setup_inputs(seed: int = 0) -> dict:
    keys = jax.random.split(jax.random.key(seed), 13)
    points = bell_draw(keys[0], (FEAT, NPTS), 1.0, 6.0, ((1, 128),))
    vectors = bell_draw(keys[1], (RHS, NPTS), 1.0, 6.0, ((0, 4), (1, 128)))
    leaf_basis = bell_draw(keys[2], (NLEAVES, LEAF, RANK), LEAF ** -0.5, 0.25, ((0, 128),))
    leaf_transfer = bell_draw(keys[3], (NLEAVES, RANK, RANK), (2 * RANK) ** -0.5, 0.375, ((0, 128),))
    node_transfer = bell_draw(keys[4], (NB, RANK, RANK), (2 * RANK) ** -0.5, 0.375, ((0, 128),))
    leaf_coupling = bell_draw(keys[5], (NLEAVES, FARL, RANK, RANK), (FARL * RANK) ** -0.5, 0.3125, ((0, 128),))
    node_coupling = bell_draw(keys[6], (NB, FARB, RANK, RANK), (FARB * RANK * LEAF_DEV // 2) ** -0.5, 0.09375, ((0, 128),))
    top_coupling = bell_draw(keys[7], (N_COL, N_COL, RANK, RANK), (NB * RANK * LEAF_DEV // 4) ** -0.5, 0.02734375, ((0, 16),))
    near_list = draw_near_list(jax.random.fold_in(keys[12], 71), 0)
    near_count = draw_near_count(jax.random.fold_in(keys[12], 71), 0)
    far_leaves = draw_far_leaves(jax.random.fold_in(keys[12], 71), 0)
    far_nodes = draw_far_nodes(jax.random.fold_in(keys[12], 71), 0)
    return {"points": points, "vectors": vectors, "leaf_basis": leaf_basis, "leaf_transfer": leaf_transfer, "node_transfer": node_transfer, "leaf_coupling": leaf_coupling, "node_coupling": node_coupling, "top_coupling": top_coupling, "near_list": near_list, "near_count": near_count, "far_leaves": far_leaves, "far_nodes": far_nodes}


def near_field(points, vectors, near_list, near_count):
    blocks = points.astype(jnp.float32).reshape(FEAT, NLEAVES, LEAF)
    columns = vectors.astype(jnp.float32).reshape(RHS, NLEAVES, LEAF)
    squares = jnp.sum(blocks * blocks, axis=0)

    def per_leaf(packed):
        leaf_id, neighbours, count_now = packed
        own_points = blocks[:, leaf_id]
        far_points = blocks[:, neighbours]
        crossed = jnp.einsum('fsb,fa->sba', far_points, own_points)
        distance = squares[neighbours][:, :, None] + squares[leaf_id][None, None, :] - 2.0 * crossed
        kernel_tile = jnp.exp(distance * (-2.0 / FEAT)).astype(jnp.bfloat16)
        kernel_tile = lax.optimization_barrier(kernel_tile).astype(jnp.float32)
        slot_mask = (jnp.arange(NEAR_MOST) < count_now).astype(jnp.float32)
        sources = columns[:, neighbours] * slot_mask[None, :, None]
        return jnp.einsum('csb,sba->ca', sources, kernel_tile)

    result = lax.map(per_leaf, (jnp.arange(NLEAVES, dtype=jnp.int32), near_list, near_count))
    return jnp.transpose(result, (1, 0, 2))


def reference(points, vectors, leaf_basis, leaf_transfer, node_transfer, leaf_coupling, node_coupling, top_coupling, near_list, near_count, far_leaves, far_nodes):
    fl = jnp.float32
    columns = vectors.shape[0]
    blocks = vectors.astype(fl).reshape(columns, NLEAVES, LEAF)
    moments = jnp.einsum('cnl,nlk->cnk', blocks, leaf_basis.astype(fl)).astype(jnp.bfloat16)
    picked = moments[:, far_leaves].astype(fl)
    leaf_field = jnp.einsum('cnkr,nkrs->cns', picked, leaf_coupling.astype(fl))
    grouped = moments.astype(fl).reshape(columns, NB, LEAF_DEV, RANK)
    transfer_grouped = leaf_transfer.astype(fl).reshape(NB, LEAF_DEV, RANK, RANK)
    node_moments = jnp.einsum('cmlr,mlrs->cms', grouped, transfer_grouped).astype(jnp.bfloat16)
    lifted = jnp.einsum('cmr,mrs->cms', node_moments.astype(fl), node_transfer.astype(fl)).astype(jnp.bfloat16)
    top_moments = jnp.sum(lifted.astype(fl).reshape(columns, N_ROW, N_COL, RANK), axis=1).astype(jnp.bfloat16)
    node_field = jnp.einsum('cmkr,mkrs->cms', node_moments[:, far_nodes].astype(fl), node_coupling.astype(fl))
    top_field = jnp.einsum('cjr,kjrs->cks', top_moments.astype(fl), top_coupling.astype(fl)).astype(jnp.bfloat16)
    spread_top = jnp.tile(top_field.astype(fl), (1, N_ROW, 1))
    node_down = (node_field + jnp.einsum('cms,mrs->cmr', spread_top, node_transfer.astype(fl))).astype(jnp.bfloat16)
    lowered = jnp.einsum('cms,mlrs->cmlr', node_down.astype(fl), transfer_grouped).reshape(columns, NLEAVES, RANK)
    leaf_down = (leaf_field + lowered).astype(jnp.bfloat16)
    far_part = jnp.einsum('cnr,nlr->cnl', leaf_down.astype(fl), leaf_basis.astype(fl))
    near_part = near_field(points, vectors, near_list, near_count)
    return (near_part + far_part).reshape(columns, NPTS).astype(jnp.bfloat16)
```

```python
import functools

import jax
import jax.numpy as jnp
from jax import lax
from jax.experimental import pallas as pl
from jax.experimental.pallas import tpu as pltpu
from jax.sharding import PartitionSpec as P

MESH = pl.DeviceIdType.MESH
LOG2E = 1.4426950408889634
f32 = jnp.float32
bf16 = jnp.bfloat16
NEAR_FIRST = (1, -1, 2, -2, 3, -3, 4)


def dot(a, b):
    return jnp.dot(a, b, preferred_element_type=f32)


def dot_nt(a, b):
    return lax.dot_general(a, b, (((1,), (1,)), ((), ())), preferred_element_type=f32)


def exchange_kernel(
    n_row,
    n_col,
    points,
    vectors,
    basis,
    transfer,
    node_transfer,
    halo_points,
    halo_vectors,
    window_moments,
    nodes_all,
    top_all,
    vec,
    bas,
    ltr,
    ntr,
    lifts,
    load_sem,
    near_node_send,
    near_node_recv,
    far_node_send,
    far_node_recv,
    lift_send,
    lift_recv,
    top_send,
    top_recv,
    pair_send,
    pair_recv,
    halo_send,
    halo_recv,
):
    n_z = n_col // 2
    row, col = lax.axis_index("row"), lax.axis_index("col")
    z, core = col // 2, col % 2
    devices = n_row * n_col
    me = row * n_col + col
    leaves = basis.shape[0]
    leaf = basis.shape[1]
    half = (leaves // 2) * leaf
    total = leaves * leaf

    def at(index):
        return {"row": index // n_col, "col": index % n_col}

    left = at((me + devices - 1) % devices)
    right = at((me + 1) % devices)
    partner = {"col": col + 1 - 2 * core}
    z_steps = [o % n_z for o in NEAR_FIRST if abs(o) <= n_z // 2]
    y_steps = [q % n_row for q in NEAR_FIRST if abs(q) <= n_row // 2]

    def z_peer(o):
        return {"col": ((z + o) % n_z) * 2 + core}

    def y_peer(q):
        return {"row": (row + q) % n_row}

    loads = [
        pltpu.make_async_copy(vectors, vec, load_sem.at[0]),
        pltpu.make_async_copy(basis, bas, load_sem.at[1]),
        pltpu.make_async_copy(transfer, ltr, load_sem.at[2]),
        pltpu.make_async_copy(node_transfer, ntr, load_sem.at[3]),
    ]
    for load in loads:
        load.start()
    barrier = pltpu.get_barrier_semaphore()
    peers = [left, right] + [z_peer(o) for o in z_steps] + [y_peer(q) for q in y_steps]
    for peer in peers:
        pl.semaphore_signal(barrier, inc=1, device_id=peer, device_id_type=MESH)

    def remote(src, dst, send, recv, device):
        return pltpu.make_async_remote_copy(
            src_ref=src,
            dst_ref=dst,
            send_sem=send,
            recv_sem=recv,
            device_id=device,
            device_id_type=MESH,
        )

    loads[0].wait()
    loads[1].wait()
    loads[2].wait()
    loads[3].wait()
    gathered = None
    for l in range(leaves):
        moment = dot(vec[:, l * leaf : (l + 1) * leaf], bas[l]).astype(bf16)
        window_moments[1, l] = moment
        part = dot(moment, ltr[l])
        gathered = part if gathered is None else gathered + part
    node = gathered.astype(bf16)
    nodes_all[core, row, z] = node
    lifts[row] = dot(node, ntr[0]).astype(bf16)
    pl.semaphore_wait(barrier, len(peers))

    started = []

    def go(copy):
        copy.start()
        started.append(copy)
        return copy

    def node_slot(o):
        return nodes_all.at[core, row, (z + n_z - o) % n_z]

    near_nodes = {}
    for o in z_steps:
        near_nodes[o] = go(
            remote(node_slot(0), node_slot(0), near_node_send.at[o], near_node_recv.at[o], z_peer(o))
        )
    far_nodes = {}

    def forward(o):
        for q in y_steps:
            far_nodes[o, q] = go(
                remote(
                    node_slot(o),
                    node_slot(o),
                    far_node_send.at[o, q],
                    far_node_recv.at[o, q],
                    y_peer(q),
                )
            )

    lifted = {}
    for q in y_steps:
        lifted[q] = go(
            remote(lifts.at[row], lifts.at[row], lift_send.at[q], lift_recv.at[q], y_peer(q))
        )
    forward(0)
    halos = []

    def send_halo(slot, src, to_left, to_right):
        halos.append(
            go(remote(src, to_left, halo_send.at[slot], halo_recv.at[slot], left))
        )
        halos.append(
            go(remote(src, to_right, halo_send.at[slot + 1], halo_recv.at[slot + 1], right))
        )

    send_halo(0, window_moments.at[1], window_moments.at[2], window_moments.at[0])
    first, second = pl.ds(0, half), pl.ds(half, total - half)
    send_halo(
        2, points.at[:, first], halo_points.at[1, :, first], halo_points.at[0, :, first]
    )
    for o in z_steps:
        near_nodes[o].wait_recv()
        forward(o)
    for q in y_steps:
        lifted[q].wait_recv()
    summed = lifts[0].astype(f32)
    for r in range(1, n_row):
        summed = summed + lifts[r].astype(f32)
    top_all[core, z] = summed.astype(bf16)
    tops = [
        go(remote(top_all.at[core, z], top_all.at[core, z], top_send.at[o], top_recv.at[o], z_peer(o)))
        for o in z_steps
    ]
    send_halo(
        4, points.at[:, second], halo_points.at[1, :, second], halo_points.at[0, :, second]
    )
    send_halo(6, vectors, halo_vectors.at[1], halo_vectors.at[0])
    pairs = []

    def give(slot, ref):
        pairs.append(go(remote(ref, ref, pair_send.at[slot], pair_recv.at[slot], partner)))

    give(0, nodes_all.at[core, row])
    for q in y_steps:
        for o in [0] + z_steps:
            far_nodes[o, q].wait_recv()
        give(q, nodes_all.at[core, (row + n_row - q) % n_row])
    for top in tops:
        top.wait_recv()
    give(n_row, top_all.at[core])
    for copy in pairs:
        copy.wait_recv()
    for copy in halos:
        copy.wait_recv()
    for copy in started:
        copy.wait_send()


def exchange(n_row, n_col, points, vectors, basis, transfer, node_transfer):
    leaves, leaf, rank = basis.shape
    columns = vectors.shape[0]
    n_z = n_col // 2
    anywhere = pl.BlockSpec(memory_space=pl.ANY)
    vmem = pl.BlockSpec(memory_space=pltpu.VMEM)
    dma = pltpu.SemaphoreType.DMA
    return pl.pallas_call(
        functools.partial(exchange_kernel, n_row, n_col),
        out_shape=(
            jax.ShapeDtypeStruct((2,) + points.shape, bf16),
            jax.ShapeDtypeStruct((2,) + vectors.shape, bf16),
            jax.ShapeDtypeStruct((3, leaves, columns, rank), bf16),
            jax.ShapeDtypeStruct((2, n_row, n_z, columns, rank), bf16),
            jax.ShapeDtypeStruct((2, n_z, columns, rank), bf16),
        ),
        in_specs=[anywhere] * 5,
        out_specs=(anywhere, anywhere, vmem, vmem, vmem),
        scratch_shapes=[
            pltpu.VMEM(vectors.shape, bf16),
            pltpu.VMEM(basis.shape, bf16),
            pltpu.VMEM(transfer.shape, bf16),
            pltpu.VMEM(node_transfer.shape, bf16),
            pltpu.VMEM((n_row, columns, rank), bf16),
            dma((4,)),
            dma((n_z,)),
            dma((n_z,)),
            dma((n_z, n_row)),
            dma((n_z, n_row)),
            dma((n_row,)),
            dma((n_row,)),
            dma((n_z,)),
            dma((n_z,)),
            dma((n_row + 1,)),
            dma((n_row + 1,)),
            dma((8,)),
            dma((8,)),
        ],
        compiler_params=pltpu.CompilerParams(collective_id=0, has_side_effects=True),
        name="exchange",
    )(points, vectors, basis, transfer, node_transfer)


def split3(value):
    high = value.astype(bf16).astype(f32)
    rest = value - high
    middle = rest.astype(bf16).astype(f32)
    return high, middle, rest - middle


def with_squares(block, scale, squares_at, ones_at, sign):
    wide = block.astype(f32)
    squares = sign * jnp.sum(wide * wide, axis=0, keepdims=True)
    high, middle, low = split3(squares)
    rows = lax.broadcasted_iota(jnp.int32, (16, block.shape[1]), 0)
    tail = jnp.where((rows >= ones_at) & (rows < ones_at + 3), sign, 0.0)
    tail = jnp.where(rows == squares_at, high, tail)
    tail = jnp.where(rows == squares_at + 1, middle, tail)
    tail = jnp.where(rows == squares_at + 2, low, tail)
    pad = jnp.zeros((128 - 16 - block.shape[0], block.shape[1]), bf16)
    return jnp.concatenate([(block * bf16(scale)), tail.astype(bf16), pad], axis=0)


def local_kernel(
    n_row,
    n_col,
    group,
    points,
    vectors,
    halo_points,
    halo_vectors,
    window_moments,
    nodes_all,
    top_all,
    basis,
    transfer,
    node_transfer,
    leaf_coupling,
    node_coupling,
    top_coupling,
    near_list,
    near_count,
    far_leaves,
    far_nodes,
    product,
    pts,
    vec,
    targets,
    near,
    mom,
    nod,
    top,
    bas,
    ltr,
    ntr,
    lcp,
    ncp,
    tcp,
    pair_target,
    pair_source,
    sem,
):
    leaves, leaf, rank = basis.shape
    features = points.shape[0]
    slots = near_list.shape[1]
    n_z = n_col // 2
    own = leaves * leaf
    me = lax.axis_index("row") * n_col + lax.axis_index("col")
    leaf_total = leaves * n_row * n_col
    window_start = (me - 1) * leaves

    def load(slot, src, dst):
        copy = pltpu.make_async_copy(src, dst, sem.at[slot])
        copy.start()
        return copy

    near_loads = [
        load(0, points, pts.at[:, pl.ds(own, own)]),
        load(1, halo_points.at[0], pts.at[:, pl.ds(0, own)]),
        load(2, halo_points.at[1], pts.at[:, pl.ds(2 * own, own)]),
        load(3, vectors, vec.at[:, pl.ds(own, own)]),
        load(4, halo_vectors.at[0], vec.at[:, pl.ds(0, own)]),
        load(5, halo_vectors.at[1], vec.at[:, pl.ds(2 * own, own)]),
    ]
    far_loads = [
        load(6, window_moments, mom),
        load(7, nodes_all, nod),
        load(8, top_all, top),
        load(9, leaf_coupling, lcp),
        load(10, node_coupling, ncp),
        load(11, top_coupling, tcp),
        load(12, node_transfer, ntr),
        load(13, transfer, ltr),
        load(14, basis, bas),
    ]

    def list_leaf(l, at):
        count = near_count[l]

        def list_slot(s, at):
            source = near_list[l, s] - window_start
            source = lax.select(source < 0, source + leaf_total, source)
            source = lax.select(source >= leaf_total, source - leaf_total, source)
            pair_target[at] = l
            pair_source[at] = source
            return at + 1

        return lax.fori_loop(0, count, list_slot, at)

    pairs = lax.fori_loop(0, leaves, list_leaf, 0)
    for extra in range(group - 1):
        pair_target[pairs + extra] = 0
        pair_source[pairs + extra] = leaves

    near[...] = jnp.zeros_like(near)
    near_loads[0].wait()

    def build(l, carry):
        at = pl.ds(pl.multiple_of(own + l * leaf, leaf), leaf)
        block = with_squares(pts[:, at], 2.0, 0, 3, -1.0)
        targets[l] = block.T
        return carry

    lax.fori_loop(0, leaves, build, 0)
    for copy in near_loads[1:]:
        copy.wait()

    tile = 256
    factor = LOG2E / (features / 2.0)

    def turn(g, carry):
        for member in range(group):
            index = g * group + member
            target = pair_target[index]
            source = pair_source[index]
            at = pl.ds(pl.multiple_of(source * leaf, leaf), leaf)
            weights = with_squares(pts[:, at], 1.0, 3, 0, 1.0)
            values = vec[:, at] * jnp.where(index < pairs, 1.0, 0.0).astype(bf16)
            for part in range(leaf // tile):
                lhs = targets[target, part * tile : (part + 1) * tile]
                kernel_tile = jnp.exp2(dot(lhs, weights) * factor).astype(bf16)
                near[target, :, part * tile : (part + 1) * tile] += dot_nt(values, kernel_tile)
        return carry

    lax.fori_loop(0, (pairs + group - 1) // group, turn, 0)

    for copy in far_loads:
        copy.wait()
    node_field = None
    for k in range(far_nodes.shape[1]):
        m = far_nodes[0, k]
        picked = nod[m % 2, m // n_col, (m % n_col) // 2]
        part = dot(picked, ncp[0, k])
        node_field = part if node_field is None else node_field + part
    top_field = None
    for j in range(n_col):
        part = dot(top[j % 2, j // 2], tcp[0, j])
        top_field = part if top_field is None else top_field + part
    node_down = (node_field + dot_nt(top_field.astype(bf16), ntr[0])).astype(bf16)
    for l in range(leaves):
        down = dot_nt(node_down, ltr[l])
        for k in range(far_leaves.shape[1]):
            j = far_leaves[l, k] - window_start
            j = lax.select(j < 0, j + leaf_total, j)
            j = lax.select(j >= leaf_total, j - leaf_total, j)
            down = down + dot(mom[j // leaves, j % leaves], lcp[l, k])
        far = dot_nt(down.astype(bf16), bas[l])
        product[:, l * leaf : (l + 1) * leaf] = (near[l] + far).astype(bf16)


def local_part(n_row, n_col, *arrays):
    (points, vectors, halo_points, halo_vectors, mom, nodes, top, basis, transfer) = arrays[:9]
    (node_transfer, leaf_coupling, node_coupling, top_coupling) = arrays[9:13]
    near_list = arrays[13]
    leaves, leaf, rank = basis.shape
    columns = vectors.shape[0]
    group = 2
    anywhere = pl.BlockSpec(memory_space=pl.ANY)
    smem = pl.BlockSpec(memory_space=pltpu.SMEM)
    vmem = pl.BlockSpec(memory_space=pltpu.VMEM)
    pairs = near_list.shape[0] * near_list.shape[1] + group
    return pl.pallas_call(
        functools.partial(local_kernel, n_row, n_col, group),
        out_shape=jax.ShapeDtypeStruct(vectors.shape, bf16),
        in_specs=[anywhere] * 13 + [smem] * 4,
        out_specs=vmem,
        scratch_shapes=[
            pltpu.VMEM((points.shape[0], 3 * points.shape[1]), bf16),
            pltpu.VMEM((columns, 3 * points.shape[1]), bf16),
            pltpu.VMEM((leaves, leaf, 128), bf16),
            pltpu.VMEM((leaves, columns, leaf), f32),
            pltpu.VMEM(mom.shape, bf16),
            pltpu.VMEM(nodes.shape, bf16),
            pltpu.VMEM(top.shape, bf16),
            pltpu.VMEM(basis.shape, bf16),
            pltpu.VMEM(transfer.shape, bf16),
            pltpu.VMEM(node_transfer.shape, bf16),
            pltpu.VMEM(leaf_coupling.shape, bf16),
            pltpu.VMEM(node_coupling.shape, bf16),
            pltpu.VMEM(top_coupling.shape, bf16),
            pltpu.SMEM((pairs,), jnp.int32),
            pltpu.SMEM((pairs,), jnp.int32),
            pltpu.SemaphoreType.DMA((15,)),
        ],
        name="local_part",
    )(*arrays)


def solution(mesh):
    n_row, n_col = mesh.shape["row"], mesh.shape["col"]

    def local(
        points,
        vectors,
        leaf_basis,
        leaf_transfer,
        node_transfer,
        leaf_coupling,
        node_coupling,
        top_coupling,
        near_list,
        near_count,
        far_leaves,
        far_nodes,
    ):
        halo_points, halo_vectors, moments, nodes, top = exchange(
            n_row, n_col, points, vectors, leaf_basis, leaf_transfer, node_transfer
        )
        return local_part(
            n_row,
            n_col,
            points,
            vectors,
            halo_points,
            halo_vectors,
            moments,
            nodes,
            top,
            leaf_basis,
            leaf_transfer,
            node_transfer,
            leaf_coupling,
            node_coupling,
            top_coupling,
            near_list,
            near_count,
            far_leaves,
            far_nodes,
        )

    return jax.shard_map(
        local,
        mesh=mesh,
        in_specs=(
            P(None, ("row", "col")),
            P("rhs", ("row", "col")),
            P(("row", "col"), None, None),
            P(("row", "col"), None, None),
            P(("row", "col"), None, None),
            P(("row", "col"), None, None, None),
            P(("row", "col"), None, None, None),
            P("col", None, None, None),
            P(("row", "col"), None),
            P(("row", "col")),
            P(("row", "col"), None),
            P(("row", "col"), None),
        ),
        out_specs=P("rhs", ("row", "col")),
        check_vma=False,
    )
```

```python
import functools

import jax
import jax.numpy as jnp
from jax import lax
from jax.experimental import pallas as pl
from jax.experimental.pallas import tpu as pltpu
from jax.sharding import PartitionSpec as P

MESH = pl.DeviceIdType.MESH
LOG2E = 1.4426950408889634
GROUP = 4
EARLY, LATE = 16, 12
f32 = jnp.float32
bf16 = jnp.bfloat16
i32 = jnp.int32
NEAR_FIRST = (1, -1, 2, -2, 3, -3, 4)


def dot(a, b):
    return jnp.dot(a, b, preferred_element_type=f32)


def dot_nt(a, b):
    return lax.dot_general(a, b, (((1,), (1,)), ((), ())), preferred_element_type=f32)


def split3(value):
    high = value.astype(bf16).astype(f32)
    rest = value - high
    middle = rest.astype(bf16).astype(f32)
    return high, middle, rest - middle


def with_squares(block, scale, squares_at, ones_at, sign):
    wide = block.astype(f32)
    squares = sign * jnp.sum(wide * wide, axis=0, keepdims=True)
    high, middle, low = split3(squares)
    rows = lax.broadcasted_iota(i32, (16, block.shape[1]), 0)
    tail = jnp.where((rows >= ones_at) & (rows < ones_at + 3), sign, 0.0)
    tail = jnp.where(rows == squares_at, high, tail)
    tail = jnp.where(rows == squares_at + 1, middle, tail)
    tail = jnp.where(rows == squares_at + 2, low, tail)
    pad = jnp.zeros((128 - 16 - block.shape[0], block.shape[1]), bf16)
    return jnp.concatenate([(block * bf16(scale)), tail.astype(bf16), pad], axis=0)


def as_target(block):
    return with_squares(block, 2.0, 0, 3, -1.0).T


def as_source(block):
    return with_squares(block, 1.0, 3, 0, 1.0)


def pair(features, target, source, values):
    factor = LOG2E / (features / 2.0)
    kernel_tile = jnp.exp2(dot(target, source) * factor).astype(bf16)
    return dot_nt(values, kernel_tile)


def place(j, me, core, devices, leaves):
    step = j // leaves - me
    is_own = step == 0
    is_right = (step == 1) | (step == 1 - devices)
    is_partner = jnp.logical_not(is_own) & (is_right == (core == 0))
    segment = jnp.where(is_own, 0, jnp.where(is_partner, 1, 2))
    return segment, j % leaves


def kernel(
    n_row,
    n_col,
    points,
    vectors,
    basis,
    transfer,
    node_transfer,
    leaf_coupling,
    node_coupling,
    top_coupling,
    near_list,
    near_count,
    far_leaves,
    far_nodes,
    partial,
    halo_points,
    halo_vectors,
    over,
    pts,
    pts_late,
    vec,
    vec_late,
    targets,
    sources,
    values,
    near,
    slots,
    mom,
    mine,
    nodes,
    top_mine,
    tops,
    lifts,
    bas,
    ltr,
    ntr,
    lcp,
    ncp,
    tcp,
    next_early,
    next_late,
    source_of,
    slot_of,
    load_sem,
    pair_send,
    pair_recv,
    lift_send,
    lift_recv,
    line_send,
    line_recv,
    far_send,
    far_recv,
    give_send,
    give_recv,
    halo_send,
    halo_recv,
):
    n_z = n_col // 2
    half = n_z // 2
    row, col = lax.axis_index("row"), lax.axis_index("col")
    z, core = col // 2, col % 2
    devices = n_row * n_col
    me = row * n_col + col
    leaves, leaf, rank = basis.shape
    features = points.shape[0]
    per_leaf = near_list.shape[0] - 1
    entries = leaves * per_leaf
    own = leaves * leaf

    def z_peer(o):
        return {"col": ((z + o) % n_z) * 2 + core}

    def y_peer(q):
        return {"row": (row + q) % n_row}

    outside = (me + devices - 1 + 2 * core) % devices
    outside = {"row": outside // n_col, "col": outside % n_col}
    partner = {"col": col + 1 - 2 * core}
    y_steps = [q % n_row for q in NEAR_FIRST if abs(q) <= n_row // 2]

    def load(slot, src, dst):
        copy = pltpu.make_async_copy(src, dst, load_sem.at[slot])
        copy.start()
        return copy

    barrier = pltpu.get_barrier_semaphore()
    peers = [partner, outside]
    peers += [z_peer(o) for o in range(1, n_z)] + [y_peer(q) for q in y_steps]
    for peer in peers:
        pl.semaphore_signal(barrier, inc=1, device_id=peer, device_id_type=MESH)
    loads = [
        load(0, vectors, vec.at[:, pl.ds(0, own)]),
        load(1, basis, bas),
        load(2, transfer, ltr),
        load(3, node_transfer, ntr),
        load(4, points, pts.at[:, pl.ds(0, own)]),
        load(5, leaf_coupling, lcp),
        load(6, node_coupling, ncp),
        load(7, top_coupling, tcp),
    ]
    started = []

    def remote(src, dst, send_sem, recv_sem, device):
        return pltpu.make_async_remote_copy(
            src_ref=src,
            dst_ref=dst,
            send_sem=send_sem,
            recv_sem=recv_sem,
            device_id=device,
            device_id_type=MESH,
        )

    def send(src, dst, send_sem, recv_sem, device):
        copy = remote(src, dst, send_sem, recv_sem, device)
        copy.start()
        started.append(copy)
        return copy

    with jax.named_scope("moments"):
        for copy in loads[:4]:
            copy.wait()
        gathered = None
        for l in range(leaves):
            moment = dot(vec[:, l * leaf : (l + 1) * leaf], bas[l]).astype(bf16)
            mom[l] = moment
            part = dot(moment, ltr[l])
            gathered = part if gathered is None else gathered + part
        node = gathered.astype(bf16)
        mine[core] = node
        lifts[row] = dot(node, ntr[0]).astype(bf16)
    with jax.named_scope("barrier"):
        pl.semaphore_wait(barrier, len(peers))

    def to_partner(slot, ref):
        return send(ref, ref, pair_send.at[slot], pair_recv.at[slot], partner)

    node_pair = to_partner(0, mine.at[core])
    lifted = [
        send(lifts.at[row], lifts.at[row], lift_send.at[q], lift_recv.at[q], y_peer(q))
        for q in y_steps
    ]

    def send_halo(slot, src, dst, device):
        return send(src, dst, halo_send.at[slot], halo_recv.at[slot], device)

    late = [send_halo(0, points, pts_late, outside), send_halo(1, vectors, vec_late, outside)]
    early = [
        send_halo(2, points, pts.at[:, pl.ds(own, own)], partner),
        send_halo(3, vectors, vec.at[:, pl.ds(own, own)], partner),
    ]
    own_moments = mom.at[pl.ds(0, leaves)]
    moments = [
        send_halo(4, own_moments, mom.at[pl.ds(leaves, leaves)], partner),
        send_halo(5, own_moments, mom.at[pl.ds(2 * leaves, leaves)], outside),
    ]

    def line_copy(stage, k, src, dst):
        step = jnp.where(core == 0, k + 1, n_z - k)
        return remote(src, dst, line_send.at[stage, k], line_recv.at[stage, k], z_peer(step))

    def line_start(stage, src, slot):
        first = line_copy(stage, 0, src, slot(0))
        last = line_copy(stage, half - 1, src, slot(half - 1))
        pl.when(core == 0)(first.start)
        pl.when(core == 1)(last.start)
        middle = [line_copy(stage, k, src, slot(k)) for k in range(1, half - 1)]
        for copy in middle:
            copy.start()
            started.append(copy)
        return [first] + middle + [last]

    def relay(stage, slot):
        k = half - 2
        return remote(
            slot(k), slot(k + 1), line_send.at[stage, k + 1], line_recv.at[stage, k + 1], z_peer(1)
        )

    with jax.named_scope("node_pair"):
        node_pair.wait_recv()

    def node_slot(k):
        return nodes.at[core, k, row]

    node_line = line_start(0, mine, node_slot)
    far = {}

    def forward_copy(k, q, src):
        return remote(src, node_slot(k), far_send.at[k, q], far_recv.at[k, q], y_peer(q))

    @pl.when(core == 1)
    def _():
        nodes[1, 0, row] = mine[...]
        for q in y_steps:
            forward_copy(0, q, mine).start()

    with jax.named_scope("lists"):
        next_early[entries] = entries
        next_late[entries] = entries
        source_of[entries] = 0

        def classify(e):
            l = e // per_leaf
            s = e % per_leaf + 1
            segment, inner = place(near_list[s, l], me, core, devices, leaves)
            used = s < near_count[l]
            return used & (segment < 2), used & (segment == 2), segment, inner

        def link(i, carry):
            e = entries - 1 - i
            is_early, is_late, segment, inner = classify(e)
            following, following_late = carry
            following = jnp.where(is_early, e, following)
            following_late = jnp.where(is_late, e, following_late)
            next_early[e] = following
            next_late[e] = following_late
            source_of[e] = segment * leaves + inner
            return following, following_late

        lax.fori_loop(0, entries, link, (i32(entries), i32(entries)))

        def number(e, carry):
            count, count_late = carry
            is_early = next_early[e] == e
            is_late = next_late[e] == e
            slot = jnp.where(is_early & (count < EARLY), count, EARLY + LATE)
            slot = jnp.where(is_late & (count_late < LATE), EARLY + count_late, slot)
            slot_of[e] = slot
            return count + jnp.where(is_early, 1, 0), count_late + jnp.where(is_late, 1, 0)

        count, count_late = lax.fori_loop(0, entries, number, (i32(0), i32(0)))
        over[0] = jnp.maximum(count - EARLY, 0) + jnp.maximum(count_late - LATE, 0)
        slots[EARLY + LATE] = jnp.zeros_like(slots[EARLY + LATE])

    with jax.named_scope("selfs"):
        loads[4].wait()

        def build(g, carry):
            for member in range(2):
                l = g * 2 + member
                targets[l] = as_target(pts[:, pl.ds(pl.multiple_of(l * leaf, leaf), leaf)])
            return carry

        lax.fori_loop(0, leaves // 2, build, 0)

        def prepare(points_from, vectors_from, start, base):
            def turn(g, carry):
                for member in range(2):
                    l = g * 2 + member
                    there = pl.ds(pl.multiple_of(start * leaf + l * leaf, leaf), leaf)
                    sources[base + l] = as_source(points_from[:, there])
                    values[base + l] = vectors_from[:, there]
                return carry

            lax.fori_loop(0, leaves // 2, turn, 0)

        prepare(pts, vec, 0, 0)

        def self_turn(g, carry):
            for member in range(GROUP):
                l = g * GROUP + member
                near[l] = pair(features, targets[l], sources[l], values[l])
            return carry

        lax.fori_loop(0, leaves // GROUP, self_turn, 0)

    with jax.named_scope("forward"):
        pl.when(core == 0)(node_line[0].wait_recv)

        @pl.when(core == 0)
        def _():
            for q in y_steps:
                forward_copy(0, q, node_slot(0)).start()

        node_line[half - 2].wait_recv()
        pl.when(core == 0)(relay(0, node_slot).start)
        for k in list(range(1, half - 2)) + [half - 1]:
            node_line[k].wait_recv()
        for k in range(1, half):
            for q in y_steps:
                copy = forward_copy(k, q, node_slot(k))
                copy.start()
                started.append(copy)
    with jax.named_scope("lifted"):
        for copy in lifted:
            copy.wait_recv()
        summed = lifts[0].astype(f32)
        for r in range(1, n_row):
            summed = summed + lifts[r].astype(f32)
        top_mine[core] = summed.astype(bf16)
        top_pair = to_partner(1, top_mine.at[core])
        for copy in early:
            copy.wait_recv()
        prepare(pts, vec, leaves, leaves)

    def list_turns(turns, base, following, start):
        def turn(g, e):
            for member in range(GROUP):
                l = jnp.minimum(e // per_leaf, leaves - 1)
                there = source_of[e]
                slots[base + g * GROUP + member] = pair(
                    features, targets[l], sources[there], values[there]
                )
                e = following[jnp.minimum(e + 1, entries)]
            return e

        return lax.fori_loop(0, turns, turn, start)

    turns = EARLY // GROUP
    first = turns // 2
    with jax.named_scope("early1"):
        at = list_turns(first, 0, next_early, next_early[0])
    with jax.named_scope("top_pair"):
        top_pair.wait_recv()

    def top_slot(k):
        return tops.at[core, k]

    top_line = line_start(1, top_mine, top_slot)

    @pl.when(core == 1)
    def _():
        tops[1, 0] = top_mine[...]

    with jax.named_scope("early2"):
        list_turns(turns - first, first * GROUP, next_early, at)
        top_line[half - 2].wait_recv()
        pl.when(core == 0)(relay(1, top_slot).start)
    for copy in loads[5:]:
        copy.wait()
    saves = [
        load(8, pts.at[:, pl.ds(own, own)], halo_points.at[0]),
        load(9, vec.at[:, pl.ds(own, own)], halo_vectors.at[0]),
    ]
    with jax.named_scope("late_wait"):
        for copy in late:
            copy.wait_recv()
        prepare(pts_late, vec_late, 0, 2 * leaves)
    saves += [load(10, pts_late, halo_points.at[1]), load(11, vec_late, halo_vectors.at[1])]
    turns = LATE // GROUP
    first = turns // 2
    with jax.named_scope("late1"):
        at = list_turns(first, EARLY, next_late, next_late[0])
    gives = []
    with jax.named_scope("give"):
        for k in range(half):
            for q in y_steps:
                forward_copy(k, q, node_slot(k)).wait_recv()
            gives.append(
                send(nodes.at[core, k], nodes.at[core, k], give_send.at[k], give_recv.at[k], partner)
            )
    with jax.named_scope("late2"):
        list_turns(turns - first, EARLY + first * GROUP, next_late, at)
    with jax.named_scope("give_top"):
        pl.when(core == 0)(top_line[0].wait_recv)
        for k in list(range(1, half - 2)) + [half - 1]:
            top_line[k].wait_recv()
        gives.append(
            send(tops.at[core], tops.at[core], give_send.at[half], give_recv.at[half], partner)
        )
        for copy in moments:
            copy.wait_recv()
    with jax.named_scope("gather"):

        def gather(l, carry):
            total = near[l]
            for s in range(per_leaf):
                total = total + slots[slot_of[l * per_leaf + s]]
            near[l] = total
            return carry

        lax.fori_loop(0, leaves, gather, 0)
    fields = []
    for l in range(leaves):
        total = None
        for k in range(far_leaves.shape[0]):
            segment, inner = place(far_leaves[k, l], me, core, devices, leaves)
            part = dot(mom[segment * leaves + inner], lcp[l, k])
            total = part if total is None else total + part
        fields.append(total)
    with jax.named_scope("gives_wait"):
        for copy in gives:
            copy.wait_recv()

    with jax.named_scope("tail"):
        node_field = None
        for k in range(far_nodes.shape[1]):
            m = far_nodes[0, k]
            step = ((m % n_col) // 2 + n_z - z) % n_z
            side = jnp.where(step < half, 1, 0)
            place_at = jnp.where(step < half, step, n_z - 1 - step)
            part = dot(nodes[side, place_at, m // n_col, m % 2], ncp[0, k])
            node_field = part if node_field is None else node_field + part
        top_field = None
        for j in range(n_col):
            step = (j // 2 + n_z - z) % n_z
            side = jnp.where(step < half, 1, 0)
            place_at = jnp.where(step < half, step, n_z - 1 - step)
            part = dot(tops[side, place_at, j % 2], tcp[0, j])
            top_field = part if top_field is None else top_field + part
        node_down = (node_field + dot_nt(top_field.astype(bf16), ntr[0])).astype(bf16)
        for l in range(leaves):
            down = (fields[l] + dot_nt(node_down, ltr[l])).astype(bf16)
            partial[l] = near[l] + dot_nt(down, bas[l])
    with jax.named_scope("ends"):
        for copy in saves:
            copy.wait()
        for copy in started:
            copy.wait_send()
        for q in y_steps:
            forward_copy(0, q, mine).wait_send()
        for line in (node_line, top_line):
            pl.when(core == 0)(line[0].wait_send)
            line[half - 1].wait_send()


def rest_kernel(
    n_row,
    n_col,
    over,
    near_list,
    near_count,
    points,
    vectors,
    halo_points,
    halo_vectors,
    partial,
    product,
    total,
    own_points,
    there_points,
    there_vectors,
    sem,
):
    col = lax.axis_index("col")
    me = lax.axis_index("row") * n_col + col
    core = col % 2
    leaves, columns, leaf = total.shape
    per_leaf = near_list.shape[0] - 1
    load = pltpu.make_async_copy(partial, total, sem.at[0])
    load.start()
    load.wait()

    @pl.when(over[0] > 0)
    def _():
        def entry(e, carry):
            count, count_late = carry
            l = e // per_leaf
            s = e % per_leaf + 1
            segment, inner = place(near_list[s, l], me, core, n_row * n_col, leaves)
            used = s < near_count[l]
            is_early, is_late = used & (segment < 2), used & (segment == 2)
            missed = (is_early & (count >= EARLY)) | (is_late & (count_late >= LATE))

            def fetch(slot, src, dst):
                copy = pltpu.make_async_copy(src, dst, sem.at[slot])
                copy.start()
                copy.wait()

            @pl.when(missed)
            def _():
                here = pl.ds(pl.multiple_of(l * leaf, leaf), leaf)
                there = pl.ds(pl.multiple_of(inner * leaf, leaf), leaf)
                fetch(0, points.at[:, here], own_points)

                @pl.when(segment == 0)
                def _():
                    fetch(1, points.at[:, there], there_points)
                    fetch(2, vectors.at[:, there], there_vectors)

                @pl.when(segment > 0)
                def _():
                    fetch(1, halo_points.at[segment - 1, :, there], there_points)
                    fetch(2, halo_vectors.at[segment - 1, :, there], there_vectors)

                target, source = as_target(own_points[...]), as_source(there_points[...])
                total[l] += pair(own_points.shape[0], target, source, there_vectors[...])

            return count + jnp.where(is_early, 1, 0), count_late + jnp.where(is_late, 1, 0)

        lax.fori_loop(0, leaves * per_leaf, entry, (i32(0), i32(0)))

    for l in range(leaves):
        product[:, l * leaf : (l + 1) * leaf] = total[l].astype(bf16)


def whole(n_row, n_col, *arrays):
    points, vectors, basis, transfer, node_transfer = arrays[:5]
    leaf_coupling, node_coupling, top_coupling, near_list, near_count = arrays[5:10]
    leaves, leaf, rank = basis.shape
    features, columns = points.shape[0], vectors.shape[0]
    own = leaves * leaf
    half = n_col // 4
    entries = leaves * (near_list.shape[0] - 1)
    anywhere = pl.BlockSpec(memory_space=pl.ANY)
    smem = pl.BlockSpec(memory_space=pltpu.SMEM)
    vmem = pl.BlockSpec(memory_space=pltpu.VMEM)
    dma = pltpu.SemaphoreType.DMA
    partial, halo_points, halo_vectors, over = pl.pallas_call(
        functools.partial(kernel, n_row, n_col),
        out_shape=(
            jax.ShapeDtypeStruct((leaves, columns, leaf), f32),
            jax.ShapeDtypeStruct((2, features, own), bf16),
            jax.ShapeDtypeStruct((2, columns, own), bf16),
            jax.ShapeDtypeStruct((1,), i32),
        ),
        in_specs=[anywhere] * 8 + [smem] * 4,
        out_specs=(vmem, anywhere, anywhere, smem),
        scratch_shapes=[
            pltpu.VMEM((features, 2 * own), bf16),
            pltpu.VMEM((features, own), bf16),
            pltpu.VMEM((columns, 2 * own), bf16),
            pltpu.VMEM((columns, own), bf16),
            pltpu.VMEM((leaves, leaf, 128), bf16),
            pltpu.VMEM((3 * leaves, 128, leaf), bf16),
            pltpu.VMEM((3 * leaves, columns, leaf), bf16),
            pltpu.VMEM((leaves, columns, leaf), f32),
            pltpu.VMEM((EARLY + LATE + 1, columns, leaf), f32),
            pltpu.VMEM((3 * leaves, columns, rank), bf16),
            pltpu.VMEM((2, columns, rank), bf16),
            pltpu.VMEM((2, half, n_row, 2, columns, rank), bf16),
            pltpu.VMEM((2, columns, rank), bf16),
            pltpu.VMEM((2, half, 2, columns, rank), bf16),
            pltpu.VMEM((n_row, columns, rank), bf16),
            pltpu.VMEM(basis.shape, bf16),
            pltpu.VMEM(transfer.shape, bf16),
            pltpu.VMEM(node_transfer.shape, bf16),
            pltpu.VMEM(leaf_coupling.shape, bf16),
            pltpu.VMEM(node_coupling.shape, bf16),
            pltpu.VMEM(top_coupling.shape, bf16),
            pltpu.SMEM((entries + 1,), i32),
            pltpu.SMEM((entries + 1,), i32),
            pltpu.SMEM((entries + 1,), i32),
            pltpu.SMEM((entries,), i32),
            dma((12,)),
            dma((2,)),
            dma((2,)),
            dma((n_row,)),
            dma((n_row,)),
            dma((2, half)),
            dma((2, half)),
            dma((half, n_row)),
            dma((half, n_row)),
            dma((half + 1,)),
            dma((half + 1,)),
            dma((6,)),
            dma((6,)),
        ],
        compiler_params=pltpu.CompilerParams(collective_id=0, has_side_effects=True),
        name="hierarchy",
    )(*arrays)
    return pl.pallas_call(
        functools.partial(rest_kernel, n_row, n_col),
        out_shape=jax.ShapeDtypeStruct(vectors.shape, bf16),
        in_specs=[smem] * 3 + [anywhere] * 5,
        out_specs=vmem,
        scratch_shapes=[
            pltpu.VMEM((leaves, columns, leaf), f32),
            pltpu.VMEM((features, leaf), bf16),
            pltpu.VMEM((features, leaf), bf16),
            pltpu.VMEM((columns, leaf), bf16),
            dma((3,)),
        ],
        name="rest",
    )(over, near_list, near_count, points, vectors, halo_points, halo_vectors, partial)


def solution(mesh):
    n_row, n_col = mesh.shape["row"], mesh.shape["col"]

    def local(
        points,
        vectors,
        leaf_basis,
        leaf_transfer,
        node_transfer,
        leaf_coupling,
        node_coupling,
        top_coupling,
        near_list,
        near_count,
        far_leaves,
        far_nodes,
    ):
        return whole(
            n_row,
            n_col,
            points,
            vectors,
            leaf_basis,
            leaf_transfer,
            node_transfer,
            leaf_coupling,
            node_coupling,
            top_coupling,
            near_list.T,
            near_count,
            far_leaves.T,
            far_nodes,
        )

    return jax.shard_map(
        local,
        mesh=mesh,
        in_specs=(
            P(None, ("row", "col")),
            P("rhs", ("row", "col")),
            P(("row", "col"), None, None),
            P(("row", "col"), None, None),
            P(("row", "col"), None, None),
            P(("row", "col"), None, None, None),
            P(("row", "col"), None, None, None),
            P("col", None, None, None),
            P(("row", "col"), None),
            P(("row", "col")),
            P(("row", "col"), None),
            P(("row", "col"), None),
        ),
        out_specs=P("rhs", ("row", "col")),
        check_vma=False,
    )
```

```python
import functools

import jax
import jax.numpy as jnp
from jax import lax
from jax.experimental import pallas as pl
from jax.experimental.pallas import tpu as pltpu
from jax.sharding import PartitionSpec as P

MESH = pl.DeviceIdType.MESH
LOG2E = 1.4426950408889634
GROUP = 4
EARLY, LATE = 20, 12
f32 = jnp.float32
bf16 = jnp.bfloat16
i32 = jnp.int32
NEAR_FIRST = (1, -1, 2, -2, 3, -3, 4)


def dot(a, b):
    return jnp.dot(a, b, preferred_element_type=f32)


def dot_nt(a, b):
    return lax.dot_general(a, b, (((1,), (1,)), ((), ())), preferred_element_type=f32)


def split3(value):
    high = value.astype(bf16).astype(f32)
    rest = value - high
    middle = rest.astype(bf16).astype(f32)
    return high, middle, rest - middle


def with_squares(block, scale, squares_at, ones_at, sign):
    wide = block.astype(f32)
    squares = sign * jnp.sum(wide * wide, axis=0, keepdims=True)
    high, middle, low = split3(squares)
    rows = lax.broadcasted_iota(i32, (16, block.shape[1]), 0)
    tail = jnp.where((rows >= ones_at) & (rows < ones_at + 3), sign, 0.0)
    tail = jnp.where(rows == squares_at, high, tail)
    tail = jnp.where(rows == squares_at + 1, middle, tail)
    tail = jnp.where(rows == squares_at + 2, low, tail)
    pad = jnp.zeros((128 - 16 - block.shape[0], block.shape[1]), bf16)
    return jnp.concatenate([(block * bf16(scale)), tail.astype(bf16), pad], axis=0)


def as_target(block):
    return with_squares(block, 2.0, 0, 3, -1.0).T


def as_source(block):
    return with_squares(block, 1.0, 3, 0, 1.0)


def pair(features, target, source, values):
    factor = LOG2E / (features / 2.0)
    kernel_tile = jnp.exp2(dot(target, source) * factor).astype(bf16)
    return dot_nt(values, kernel_tile)


def place(j, me, core, devices, leaves):
    step = j // leaves - me
    is_own = step == 0
    is_right = (step == 1) | (step == 1 - devices)
    is_partner = jnp.logical_not(is_own) & (is_right == (core == 0))
    segment = jnp.where(is_own, 0, jnp.where(is_partner, 1, 2))
    return segment, j % leaves


def kernel(
    n_row,
    n_col,
    n_rhs,
    points,
    vectors,
    basis,
    transfer,
    node_transfer,
    leaf_coupling,
    node_coupling,
    top_coupling,
    near_list_in,
    near_count_in,
    far_leaves_in,
    far_nodes_in,
    partial,
    halo_points,
    halo_vectors,
    over,
    result,
    near_list,
    near_count,
    far_leaves,
    far_nodes,
    pts,
    pts_late,
    vec,
    vec_late,
    targets,
    sources,
    values,
    near,
    slots,
    mom,
    mine,
    line,
    nodes,
    lifted,
    top_parts,
    bas,
    ltr,
    ntr,
    lcp,
    ncp,
    tcp,
    next_early,
    next_late,
    source_of,
    slot_of,
    load_sem,
    pair_send,
    pair_recv,
    top_send,
    top_recv,
    line_send,
    line_recv,
    far_send,
    far_recv,
    give_send,
    give_recv,
    halo_send,
    halo_recv,
    share_send,
    share_recv,
):
    n_z = n_col // 2
    half = n_z // 2
    row, col = lax.axis_index("row"), lax.axis_index("col")
    z, core = col // 2, col % 2
    devices = n_row * n_col
    me = row * n_col + col
    leaves, leaf, rank = basis.shape
    features = points.shape[0]
    per_leaf = near_list.shape[0] - 1
    entries = leaves * per_leaf
    own = leaves * leaf

    def z_peer(o):
        return {"col": ((z + o) % n_z) * 2 + core}

    def y_peer(q):
        return {"row": (row + q) % n_row}

    outside = (me + devices - 1 + 2 * core) % devices
    outside = {"row": outside // n_col, "col": outside % n_col}
    partner = {"col": col + 1 - 2 * core}
    y_steps = [q % n_row for q in NEAR_FIRST if abs(q) <= n_row // 2]

    def load(slot, src, dst):
        copy = pltpu.make_async_copy(src, dst, load_sem.at[slot])
        copy.start()
        return copy

    barrier = pltpu.get_barrier_semaphore()
    peers = [partner, outside]
    peers += [z_peer(o) for o in range(1, n_z)] + [y_peer(q) for q in y_steps]
    x = lax.axis_index("rhs")
    x_peers = {d: {"rhs": (x + d) % n_rhs} for d in range(1, n_rhs)}
    peers += list(x_peers.values())
    crosses = ((core == 0) & (z == 0)) | ((core == 1) & (z == n_z - 1))
    stays = jnp.logical_not(crosses)
    for peer in peers:
        pl.semaphore_signal(barrier, inc=1, device_id=peer, device_id_type=MESH)
    chunk = leaves // 4
    vectors_load = load(0, vectors, vec.at[:, pl.ds(0, own)])
    basis_loads = [
        load(1 + c, basis.at[pl.ds(c * chunk, chunk)], bas.at[pl.ds(c * chunk, chunk)])
        for c in range(4)
    ]
    transfer_loads = [load(5, transfer, ltr), load(6, node_transfer, ntr)]
    points_load = load(7, points, pts.at[:, pl.ds(0, own)])
    list_loads = [
        load(8, near_list_in, near_list),
        load(9, near_count_in, near_count),
        load(10, far_leaves_in, far_leaves),
        load(11, far_nodes_in, far_nodes),
    ]
    coupling_loads = [
        load(12, leaf_coupling, lcp),
        load(13, node_coupling, ncp),
        load(14, top_coupling, tcp),
    ]
    started = []

    def remote(src, dst, send_sem, recv_sem, device):
        return pltpu.make_async_remote_copy(
            src_ref=src,
            dst_ref=dst,
            send_sem=send_sem,
            recv_sem=recv_sem,
            device_id=device,
            device_id_type=MESH,
        )

    def send(src, dst, send_sem, recv_sem, device):
        copy = remote(src, dst, send_sem, recv_sem, device)
        copy.start()
        started.append(copy)
        return copy

    with jax.named_scope("moments"):
        vectors_load.wait()
        here = []
        for l in range(leaves):
            if l % chunk == 0:
                basis_loads[l // chunk].wait()
            here.append(dot(vec[:, l * leaf : (l + 1) * leaf], bas[l]).astype(bf16))
            mom[l] = here[l]
        for copy in transfer_loads:
            copy.wait()
        gathered = None
        for l in range(leaves):
            part = dot(here[l], ltr[l])
            gathered = part if gathered is None else gathered + part
        node = gathered.astype(bf16)
        mine[0, core] = node
        mine[1, core] = dot(node, ntr[0]).astype(bf16)
    with jax.named_scope("barrier"):
        pl.semaphore_wait(barrier, len(peers))

    own_pair = mine.at[:, core]
    node_pair = send(own_pair, own_pair, pair_send.at[0], pair_recv.at[0], partner)

    def send_halo(slot, src, dst, device):
        return send(src, dst, halo_send.at[slot], halo_recv.at[slot], device)

    early = [
        send_halo(2, points, pts.at[:, pl.ds(own, own)], partner),
        send_halo(3, vectors, vec.at[:, pl.ds(own, own)], partner),
    ]
    own_moments = mom.at[pl.ds(0, leaves)]
    moments = [send_halo(4, own_moments, mom.at[pl.ds(leaves, leaves)], partner)]

    def line_copy(k):
        step = jnp.where(core == 0, k + 1, n_z - k)
        return remote(mine, line.at[k], line_send.at[k], line_recv.at[k], z_peer(step))

    lines = [line_copy(k) for k in range(half)]
    last = half - 1
    relay = remote(
        line.at[last - 1], line.at[last], line_send.at[last], line_recv.at[last], z_peer(1)
    )
    far = {}
    for k in range(half):
        for q in y_steps:
            far[k, q] = remote(
                line.at[k, 0],
                nodes.at[core, k, row],
                far_send.at[k, q],
                far_recv.at[k, q],
                y_peer(q),
            )

    def forward(k):
        for q in y_steps:
            far[k, q].start()
        nodes[core, k, row] = line[k, 0]

    with jax.named_scope("node_pair"):
        node_pair.wait_recv()
    pl.when(core == 0)(lines[0].start)
    for k in range(1, last):
        lines[k].start()

    @pl.when(core == 1)
    def _():
        lines[last].start()
        line[0] = mine[...]
        for q in y_steps:
            remote(
                mine.at[0], nodes.at[core, 0, row], far_send.at[0, q], far_recv.at[0, q], y_peer(q)
            ).start()
        nodes[1, 0, row] = mine[0]

    part = (leaves // 2) * leaf
    rest = pl.ds(part, own - part)
    halves = [
        remote(points.at[:, r], pts_late.at[:, r], halo_send.at[i], halo_recv.at[i], outside)
        for i, r in enumerate((pl.ds(0, part), rest))
    ]
    width = own // n_rhs
    share = pl.ds(pl.multiple_of(x * width, width), width)
    shared = pts_late.at[:, share]
    quarter = remote(points.at[:, share], shared, halo_send.at[7], halo_recv.at[7], outside)
    copies = [
        remote(shared, shared, share_send.at[d], share_recv.at[d], peer)
        for d, peer in x_peers.items()
    ]
    pl.when(stays)(halves[0].start)
    pl.when(crosses)(quarter.start)
    with jax.named_scope("lists"):
        for copy in list_loads:
            copy.wait()
        next_early[entries] = entries
        next_late[entries] = entries
        source_of[entries] = 0

        def classify(e):
            l = e // per_leaf
            s = e % per_leaf + 1
            segment, inner = place(near_list[s, l], me, core, devices, leaves)
            used = s < near_count[l]
            return used & (segment < 2), used & (segment == 2), segment, inner

        def link(i, carry):
            e = entries - 1 - i
            is_early, is_late, segment, inner = classify(e)
            following, following_late = carry
            following = jnp.where(is_early, e, following)
            following_late = jnp.where(is_late, e, following_late)
            next_early[e] = following
            next_late[e] = following_late
            source_of[e] = segment * leaves + inner
            return following, following_late

        lax.fori_loop(0, entries, link, (i32(entries), i32(entries)))

        def number(e, carry):
            count, count_late = carry
            is_early = next_early[e] == e
            is_late = next_late[e] == e
            slot = jnp.where(is_early & (count < EARLY), count, EARLY + LATE)
            slot = jnp.where(is_late & (count_late < LATE), EARLY + count_late, slot)
            slot_of[e] = slot
            return count + jnp.where(is_early, 1, 0), count_late + jnp.where(is_late, 1, 0)

        count, count_late = lax.fori_loop(0, entries, number, (i32(0), i32(0)))
        over[0] = jnp.maximum(count - EARLY, 0) + jnp.maximum(count_late - LATE, 0)
        slots[EARLY + LATE] = jnp.zeros_like(slots[EARLY + LATE])

    with jax.named_scope("selfs"):
        points_load.wait()

        def build(g, carry):
            for member in range(2):
                l = g * 2 + member
                targets[l] = as_target(pts[:, pl.ds(pl.multiple_of(l * leaf, leaf), leaf)])
            return carry

        lax.fori_loop(0, leaves // 2, build, 0)

        def prepare(points_from, vectors_from, start, base):
            def turn(g, carry):
                for member in range(2):
                    l = g * 2 + member
                    there = pl.ds(pl.multiple_of(start * leaf + l * leaf, leaf), leaf)
                    sources[base + l] = as_source(points_from[:, there])
                    values[base + l] = vectors_from[:, there]
                return carry

            lax.fori_loop(0, leaves // 2, turn, 0)

        prepare(pts, vec, 0, 0)

    def self_turn(g, carry):
        for member in range(GROUP):
            l = g * GROUP + member
            near[l] = pair(features, targets[l], sources[l], values[l])
        return carry

    pl.when(stays)(halves[1].start)
    late_vectors = send_halo(5, vectors, vec_late, outside)
    with jax.named_scope("self1"):
        lax.fori_loop(0, 2, self_turn, 0)
    with jax.named_scope("relay"):
        lines[last - 1].wait_recv()
        pl.when(core == 0)(relay.start)
    with jax.named_scope("forward1"):
        pl.when(core == 0)(lines[0].wait_recv)
        for k in range(1, last - 1):
            lines[k].wait_recv()
        pl.when(core == 0)(lambda: forward(0))
        for k in range(1, last):
            forward(k)
    with jax.named_scope("self2"):
        lax.fori_loop(2, leaves // GROUP, self_turn, 0)
    with jax.named_scope("quarter"):

        @pl.when(crosses)
        def _():
            quarter.wait_recv()
            for copy in copies:
                copy.start()

        moments.append(send_halo(6, own_moments, mom.at[pl.ds(2 * leaves, leaves)], outside))

    def list_turns(turns, base, following, start):
        def turn(g, e):
            for member in range(GROUP):
                l = jnp.minimum(e // per_leaf, leaves - 1)
                there = source_of[e]
                slots[base + g * GROUP + member] = pair(
                    features, targets[l], sources[there], values[there]
                )
                e = following[jnp.minimum(e + 1, entries)]
            return e

        return lax.fori_loop(0, turns, turn, start)

    with jax.named_scope("early"):
        for copy in early:
            copy.wait_recv()
        prepare(pts, vec, leaves, leaves)
        at = list_turns(2, 0, next_early, next_early[0])
    with jax.named_scope("forward2"):
        lines[last].wait_recv()
        forward(last)
        lifted_pair = send(line.at[:, 1], lifted, pair_send.at[1], pair_recv.at[1], partner)
    with jax.named_scope("early2"):
        list_turns(EARLY // GROUP - 2, 2 * GROUP, next_early, at)
    with jax.named_scope("top_part"):
        for copy in coupling_loads:
            copy.wait()
        lifted_pair.wait_recv()
        top_part = None
        for k in range(half):
            below, above = (z + n_z - k - 1) % n_z, (z + k) % n_z
            near_z = jnp.where(core == 0, below, above)
            other_z = jnp.where(core == 0, above, below)
            for c in range(2):
                part = dot(line[k, 1, c], tcp[0, 2 * near_z + c])
                top_part = part if top_part is None else top_part + part
                top_part = top_part + dot(lifted[k, c], tcp[0, 2 * other_z + c])
        top_parts[row] = top_part
        top_sends = [
            send(top_parts.at[row], top_parts.at[row], top_send.at[q], top_recv.at[q], y_peer(q))
            for q in y_steps
        ]
    saves = [
        load(15, pts.at[:, pl.ds(own, own)], halo_points.at[0]),
        load(16, vec.at[:, pl.ds(own, own)], halo_vectors.at[0]),
    ]
    with jax.named_scope("late_wait"):
        late_vectors.wait_recv()

        @pl.when(stays)
        def _():
            for copy in halves:
                copy.wait_recv()

        @pl.when(crosses)
        def _():
            for copy in copies:
                copy.wait_recv()

        prepare(pts_late, vec_late, 0, 2 * leaves)
    saves += [load(17, pts_late, halo_points.at[1]), load(18, vec_late, halo_vectors.at[1])]
    with jax.named_scope("late"):
        at = list_turns(2, EARLY, next_late, next_late[0])
    gives = []
    with jax.named_scope("give"):
        for k in range(half):
            for q in y_steps:
                far[k, q].wait_recv()
            ref = nodes.at[core, k]
            gives.append(send(ref, ref, give_send.at[k], give_recv.at[k], partner))
    with jax.named_scope("late2"):
        list_turns(LATE // GROUP - 2, EARLY + 2 * GROUP, next_late, at)
        for copy in moments:
            copy.wait_recv()
    with jax.named_scope("gather"):

        def gather(l, carry):
            total = near[l]
            for s in range(per_leaf):
                total = total + slots[slot_of[l * per_leaf + s]]
            near[l] = total
            return carry

        lax.fori_loop(0, leaves, gather, 0)
    fields = []
    for l in range(leaves):
        total = None
        for k in range(far_leaves.shape[0]):
            segment, inner = place(far_leaves[k, l], me, core, devices, leaves)
            part = dot(mom[segment * leaves + inner], lcp[l, k])
            total = part if total is None else total + part
        fields.append(total)
    with jax.named_scope("gives_wait"):
        for copy in top_sends:
            copy.wait_recv()
        for copy in gives:
            copy.wait_recv()

    with jax.named_scope("tail"):
        node_field = None
        for k in range(far_nodes.shape[1]):
            m = far_nodes[0, k]
            step = ((m % n_col) // 2 + n_z - z) % n_z
            side = jnp.where(step < half, 1, 0)
            place_at = jnp.where(step < half, step, n_z - 1 - step)
            part = dot(nodes[side, place_at, m // n_col, m % 2], ncp[0, k])
            node_field = part if node_field is None else node_field + part
        top_field = top_parts[0]
        for r in range(1, n_row):
            top_field = top_field + top_parts[r]
        node_down = (node_field + dot_nt(top_field.astype(bf16), ntr[0])).astype(bf16)
        for l in range(leaves):
            down = (fields[l] + dot_nt(node_down, ltr[l])).astype(bf16)
            result[l] = near[l] + dot_nt(down, bas[l])
            if (l + 1) % chunk == 0:
                done = pl.ds(l + 1 - chunk, chunk)
                saves.append(load(19 + l // chunk, result.at[done], partial.at[done]))
    with jax.named_scope("ends"):
        for copy in saves:
            copy.wait()
        for copy in started:
            copy.wait_send()
        for copy in far.values():
            copy.wait_send()
        pl.when(core == 0)(lines[0].wait_send)

        @pl.when(stays)
        def _():
            for copy in halves:
                copy.wait_send()

        @pl.when(crosses)
        def _():
            for copy in [quarter] + copies:
                copy.wait_send()

        for k in range(1, half):
            lines[k].wait_send()


def rest_kernel(
    n_row,
    n_col,
    over,
    near_list_in,
    near_count_in,
    points,
    vectors,
    halo_points,
    halo_vectors,
    partial,
    product,
    near_list,
    near_count,
    total,
    rounded,
    own_points,
    there_points,
    there_vectors,
    sem,
    chunk_sem,
):
    col = lax.axis_index("col")
    me = lax.axis_index("row") * n_col + col
    core = col % 2
    leaves, columns, leaf = total.shape
    per_leaf = near_list.shape[0] - 1
    chunk = leaves // 4
    loads = []
    for c in range(4):
        part = pl.ds(c * chunk, chunk)
        loads.append(pltpu.make_async_copy(partial.at[part], total.at[part], chunk_sem.at[c]))
        loads[c].start()

    def store(c):
        span = pl.ds(c * chunk * leaf, chunk * leaf)
        return pltpu.make_async_copy(
            rounded.at[:, span], product.at[:, span], chunk_sem.at[4 + c]
        )

    def finish(c):
        for l in range(c * chunk, (c + 1) * chunk):
            rounded[:, l * leaf : (l + 1) * leaf] = total[l].astype(bf16)
        store(c).start()

    @pl.when(over[0] == 0)
    def _():
        for c in range(4):
            loads[c].wait()
            finish(c)

    @pl.when(over[0] > 0)
    def _():
        lists = [
            pltpu.make_async_copy(near_list_in, near_list, sem.at[0]),
            pltpu.make_async_copy(near_count_in, near_count, sem.at[1]),
        ]
        for copy in lists:
            copy.start()
        for copy in lists + loads:
            copy.wait()
        def entry(e, carry):
            count, count_late = carry
            l = e // per_leaf
            s = e % per_leaf + 1
            segment, inner = place(near_list[s, l], me, core, n_row * n_col, leaves)
            used = s < near_count[l]
            is_early, is_late = used & (segment < 2), used & (segment == 2)
            missed = (is_early & (count >= EARLY)) | (is_late & (count_late >= LATE))

            def fetch(slot, src, dst):
                copy = pltpu.make_async_copy(src, dst, sem.at[slot])
                copy.start()
                copy.wait()

            @pl.when(missed)
            def _():
                here = pl.ds(pl.multiple_of(l * leaf, leaf), leaf)
                there = pl.ds(pl.multiple_of(inner * leaf, leaf), leaf)
                fetch(0, points.at[:, here], own_points)

                @pl.when(segment == 0)
                def _():
                    fetch(1, points.at[:, there], there_points)
                    fetch(2, vectors.at[:, there], there_vectors)

                @pl.when(segment > 0)
                def _():
                    fetch(1, halo_points.at[segment - 1, :, there], there_points)
                    fetch(2, halo_vectors.at[segment - 1, :, there], there_vectors)

                target, source = as_target(own_points[...]), as_source(there_points[...])
                total[l] += pair(own_points.shape[0], target, source, there_vectors[...])

            return count + jnp.where(is_early, 1, 0), count_late + jnp.where(is_late, 1, 0)

        lax.fori_loop(0, leaves * per_leaf, entry, (i32(0), i32(0)))
        for c in range(4):
            finish(c)

    for c in range(4):
        store(c).wait()


def whole(n_row, n_col, n_rhs, *arrays):
    points, vectors, basis, transfer, node_transfer = arrays[:5]
    leaf_coupling, node_coupling, top_coupling, near_list, near_count, far_leaves, far_nodes = arrays[5:12]
    leaves, leaf, rank = basis.shape
    features, columns = points.shape[0], vectors.shape[0]
    own = leaves * leaf
    half = n_col // 4
    entries = leaves * (near_list.shape[0] - 1)
    anywhere = pl.BlockSpec(memory_space=pl.ANY)
    smem = pl.BlockSpec(memory_space=pltpu.SMEM)
    dma = pltpu.SemaphoreType.DMA
    partial, halo_points, halo_vectors, over = pl.pallas_call(
        functools.partial(kernel, n_row, n_col, n_rhs),
        out_shape=(
            jax.ShapeDtypeStruct((leaves, columns, leaf), f32),
            jax.ShapeDtypeStruct((2, features, own), bf16),
            jax.ShapeDtypeStruct((2, columns, own), bf16),
            jax.ShapeDtypeStruct((1,), i32),
        ),
        in_specs=[anywhere] * 12,
        out_specs=(anywhere, anywhere, anywhere, smem),
        scratch_shapes=[
            pltpu.VMEM((leaves, columns, leaf), f32),
            pltpu.SMEM(near_list.shape, i32),
            pltpu.SMEM(near_count.shape, i32),
            pltpu.SMEM(far_leaves.shape, i32),
            pltpu.SMEM(far_nodes.shape, i32),
            pltpu.VMEM((features, 2 * own), bf16),
            pltpu.VMEM((features, own), bf16),
            pltpu.VMEM((columns, 2 * own), bf16),
            pltpu.VMEM((columns, own), bf16),
            pltpu.VMEM((leaves, leaf, 128), bf16),
            pltpu.VMEM((3 * leaves, 128, leaf), bf16),
            pltpu.VMEM((3 * leaves, columns, leaf), bf16),
            pltpu.VMEM((leaves, columns, leaf), f32),
            pltpu.VMEM((EARLY + LATE + 1, columns, leaf), f32),
            pltpu.VMEM((3 * leaves, columns, rank), bf16),
            pltpu.VMEM((2, 2, columns, rank), bf16),
            pltpu.VMEM((half, 2, 2, columns, rank), bf16),
            pltpu.VMEM((2, half, n_row, 2, columns, rank), bf16),
            pltpu.VMEM((half, 2, columns, rank), bf16),
            pltpu.VMEM((n_row, columns, rank), f32),
            pltpu.VMEM(basis.shape, bf16),
            pltpu.VMEM(transfer.shape, bf16),
            pltpu.VMEM(node_transfer.shape, bf16),
            pltpu.VMEM(leaf_coupling.shape, bf16),
            pltpu.VMEM(node_coupling.shape, bf16),
            pltpu.VMEM(top_coupling.shape, bf16),
            pltpu.SMEM((entries + 1,), i32),
            pltpu.SMEM((entries + 1,), i32),
            pltpu.SMEM((entries + 1,), i32),
            pltpu.SMEM((entries,), i32),
            dma((23,)),
            dma((2,)),
            dma((2,)),
            dma((n_row,)),
            dma((n_row,)),
            dma((half,)),
            dma((half,)),
            dma((half, n_row)),
            dma((half, n_row)),
            dma((half,)),
            dma((half,)),
            dma((8,)),
            dma((8,)),
            dma((n_rhs,)),
            dma((n_rhs,)),
        ],
        compiler_params=pltpu.CompilerParams(collective_id=0, has_side_effects=True),
        name="hierarchy",
    )(*arrays)
    return pl.pallas_call(
        functools.partial(rest_kernel, n_row, n_col),
        out_shape=jax.ShapeDtypeStruct(vectors.shape, bf16),
        in_specs=[smem] + [anywhere] * 7,
        out_specs=anywhere,
        scratch_shapes=[
            pltpu.SMEM(near_list.shape, i32),
            pltpu.SMEM(near_count.shape, i32),
            pltpu.VMEM((leaves, columns, leaf), f32),
            pltpu.VMEM(vectors.shape, bf16),
            pltpu.VMEM((features, leaf), bf16),
            pltpu.VMEM((features, leaf), bf16),
            pltpu.VMEM((columns, leaf), bf16),
            dma((3,)),
            dma((8,)),
        ],
        name="rest",
    )(over, near_list, near_count, points, vectors, halo_points, halo_vectors, partial)


def solution(mesh):
    n_row, n_col, n_rhs = mesh.shape["row"], mesh.shape["col"], mesh.shape["rhs"]

    def local(
        points,
        vectors,
        leaf_basis,
        leaf_transfer,
        node_transfer,
        leaf_coupling,
        node_coupling,
        top_coupling,
        near_list,
        near_count,
        far_leaves,
        far_nodes,
    ):
        return whole(
            n_row,
            n_col,
            n_rhs,
            points,
            vectors,
            leaf_basis,
            leaf_transfer,
            node_transfer,
            leaf_coupling,
            node_coupling,
            top_coupling,
            near_list.T,
            near_count,
            far_leaves.T,
            far_nodes,
        )

    return jax.shard_map(
        local,
        mesh=mesh,
        in_specs=(
            P(None, ("row", "col")),
            P("rhs", ("row", "col")),
            P(("row", "col"), None, None),
            P(("row", "col"), None, None),
            P(("row", "col"), None, None),
            P(("row", "col"), None, None, None),
            P(("row", "col"), None, None, None),
            P("col", None, None, None),
            P(("row", "col"), None),
            P(("row", "col")),
            P(("row", "col"), None),
            P(("row", "col"), None),
        ),
        out_specs=P("rhs", ("row", "col")),
        check_vma=False,
    )
```

```python
import functools

import jax
import jax.numpy as jnp
from jax import lax
from jax.experimental import pallas as pl
from jax.experimental.pallas import tpu as pltpu
from jax.sharding import PartitionSpec as P

MESH = pl.DeviceIdType.MESH
LOG2E = 1.4426950408889634
GROUP = 4
EARLY, LATE = 20, 12
f32 = jnp.float32
bf16 = jnp.bfloat16
i32 = jnp.int32
NEAR_FIRST = (1, -1, 2, -2, 3, -3, 4)


def dot(a, b):
    return jnp.dot(a, b, preferred_element_type=f32)


def dot_nt(a, b):
    return lax.dot_general(a, b, (((1,), (1,)), ((), ())), preferred_element_type=f32)


def split3(value):
    high = value.astype(bf16).astype(f32)
    rest = value - high
    middle = rest.astype(bf16).astype(f32)
    return high, middle, rest - middle


def with_squares(block, scale, squares_at, ones_at, sign):
    wide = block.astype(f32)
    squares = sign * jnp.sum(wide * wide, axis=0, keepdims=True)
    high, middle, low = split3(squares)
    rows = lax.broadcasted_iota(i32, (16, block.shape[1]), 0)
    tail = jnp.where((rows >= ones_at) & (rows < ones_at + 3), sign, 0.0)
    tail = jnp.where(rows == squares_at, high, tail)
    tail = jnp.where(rows == squares_at + 1, middle, tail)
    tail = jnp.where(rows == squares_at + 2, low, tail)
    pad = jnp.zeros((128 - 16 - block.shape[0], block.shape[1]), bf16)
    return jnp.concatenate([(block * bf16(scale)), tail.astype(bf16), pad], axis=0)


def as_target(block):
    return with_squares(block, 2.0, 0, 3, -1.0).T


def as_source(block):
    return with_squares(block, 1.0, 3, 0, 1.0)


def pair(features, target, source, values):
    factor = LOG2E / (features / 2.0)
    kernel_tile = jnp.exp2(dot(target, source) * factor).astype(bf16)
    return dot_nt(values, kernel_tile)


def place(j, me, core, devices, leaves):
    step = j // leaves - me
    is_own = step == 0
    is_right = (step == 1) | (step == 1 - devices)
    is_partner = jnp.logical_not(is_own) & (is_right == (core == 0))
    segment = jnp.where(is_own, 0, jnp.where(is_partner, 1, 2))
    return segment, j % leaves


def kernel(
    n_row,
    n_col,
    n_rhs,
    points,
    vectors,
    basis,
    transfer,
    node_transfer,
    leaf_coupling,
    node_coupling,
    top_coupling,
    near_list_in,
    near_count_in,
    far_leaves_in,
    far_nodes_in,
    partial,
    halo_points,
    halo_vectors,
    over,
    result,
    near_list,
    near_count,
    far_leaves,
    far_nodes,
    pts,
    pts_late,
    vec,
    vec_late,
    targets,
    sources,
    values,
    near,
    slots,
    mom,
    mine,
    line,
    nodes,
    lifted,
    top_parts,
    bas,
    ltr,
    ntr,
    lcp,
    ncp,
    tcp,
    next_early,
    next_late,
    source_of,
    slot_of,
    load_sem,
    pair_send,
    pair_recv,
    top_send,
    top_recv,
    line_send,
    line_recv,
    far_send,
    far_recv,
    give_send,
    give_recv,
    halo_send,
    halo_recv,
    share_send,
    share_recv,
):
    n_z = n_col // 2
    half = n_z // 2
    row, col = lax.axis_index("row"), lax.axis_index("col")
    z, core = col // 2, col % 2
    devices = n_row * n_col
    me = row * n_col + col
    leaves, leaf, rank = basis.shape
    features = points.shape[0]
    per_leaf = near_list.shape[0] - 1
    entries = leaves * per_leaf
    own = leaves * leaf

    def z_peer(o):
        return {"col": ((z + o) % n_z) * 2 + core}

    def y_peer(q):
        return {"row": (row + q) % n_row}

    outside = (me + devices - 1 + 2 * core) % devices
    outside = {"row": outside // n_col, "col": outside % n_col}
    partner = {"col": col + 1 - 2 * core}
    y_steps = [q % n_row for q in NEAR_FIRST if abs(q) <= n_row // 2]

    def load(slot, src, dst):
        copy = pltpu.make_async_copy(src, dst, load_sem.at[slot])
        copy.start()
        return copy

    barrier = pltpu.get_barrier_semaphore()
    peers = [partner, outside]
    peers += [z_peer(o) for o in range(1, n_z)] + [y_peer(q) for q in y_steps]
    x = lax.axis_index("rhs")
    x_peers = {d: {"rhs": (x + d) % n_rhs} for d in range(1, n_rhs)}
    peers += list(x_peers.values())
    crosses = ((core == 0) & (z == 0)) | ((core == 1) & (z == n_z - 1))
    stays = jnp.logical_not(crosses)
    for peer in peers:
        pl.semaphore_signal(barrier, inc=1, device_id=peer, device_id_type=MESH)
    chunk = leaves // 4
    vectors_load = load(0, vectors, vec.at[:, pl.ds(0, own)])
    basis_loads = [
        load(1 + c, basis.at[pl.ds(c * chunk, chunk)], bas.at[pl.ds(c * chunk, chunk)])
        for c in range(4)
    ]
    transfer_loads = [load(5, transfer, ltr), load(6, node_transfer, ntr)]
    points_load = load(7, points, pts.at[:, pl.ds(0, own)])
    list_loads = [
        load(8, near_list_in, near_list),
        load(9, near_count_in, near_count),
        load(10, far_leaves_in, far_leaves),
        load(11, far_nodes_in, far_nodes),
    ]
    coupling_loads = [
        load(12, leaf_coupling, lcp),
        load(13, node_coupling, ncp),
        load(14, top_coupling, tcp),
    ]
    started = []

    def remote(src, dst, send_sem, recv_sem, device):
        return pltpu.make_async_remote_copy(
            src_ref=src,
            dst_ref=dst,
            send_sem=send_sem,
            recv_sem=recv_sem,
            device_id=device,
            device_id_type=MESH,
        )

    def send(src, dst, send_sem, recv_sem, device):
        copy = remote(src, dst, send_sem, recv_sem, device)
        copy.start()
        started.append(copy)
        return copy

    with jax.named_scope("moments"):
        vectors_load.wait()
        here = []
        for l in range(leaves):
            if l % chunk == 0:
                basis_loads[l // chunk].wait()
            here.append(dot(vec[:, l * leaf : (l + 1) * leaf], bas[l]).astype(bf16))
            mom[l] = here[l]
        for copy in transfer_loads:
            copy.wait()
        gathered = None
        for l in range(leaves):
            part = dot(here[l], ltr[l])
            gathered = part if gathered is None else gathered + part
        node = gathered.astype(bf16)
        mine[0, core] = node
        mine[1, core] = dot(node, ntr[0]).astype(bf16)
    with jax.named_scope("barrier"):
        pl.semaphore_wait(barrier, len(peers))

    own_pair = mine.at[:, core]
    node_pair = send(own_pair, own_pair, pair_send.at[0], pair_recv.at[0], partner)

    def send_halo(slot, src, dst, device):
        return send(src, dst, halo_send.at[slot], halo_recv.at[slot], device)

    early = [
        send_halo(2, points, pts.at[:, pl.ds(own, own)], partner),
        send_halo(3, vectors, vec.at[:, pl.ds(own, own)], partner),
    ]
    own_moments = mom.at[pl.ds(0, leaves)]
    moments = [send_halo(4, own_moments, mom.at[pl.ds(leaves, leaves)], partner)]

    def line_copy(k):
        step = jnp.where(core == 0, k + 1, n_z - k)
        return remote(mine, line.at[k], line_send.at[k], line_recv.at[k], z_peer(step))

    lines = [line_copy(k) for k in range(half)]
    last = half - 1
    relay = remote(
        line.at[last - 1], line.at[last], line_send.at[last], line_recv.at[last], z_peer(1)
    )
    far = {}
    for k in range(half):
        for q in y_steps:
            far[k, q] = remote(
                line.at[k, 0],
                nodes.at[core, k, row],
                far_send.at[k, q],
                far_recv.at[k, q],
                y_peer(q),
            )

    def forward(k):
        for q in y_steps:
            far[k, q].start()
        nodes[core, k, row] = line[k, 0]

    with jax.named_scope("node_pair"):
        node_pair.wait_recv()
    pl.when(core == 0)(lines[0].start)
    for k in range(1, last):
        lines[k].start()

    @pl.when(core == 1)
    def _():
        lines[last].start()
        line[0] = mine[...]
        for q in y_steps:
            remote(
                mine.at[0], nodes.at[core, 0, row], far_send.at[0, q], far_recv.at[0, q], y_peer(q)
            ).start()
        nodes[1, 0, row] = mine[0]

    part = (leaves // 2) * leaf
    rest = pl.ds(part, own - part)
    halves = [
        remote(points.at[:, r], pts_late.at[:, r], halo_send.at[i], halo_recv.at[i], outside)
        for i, r in enumerate((pl.ds(0, part), rest))
    ]
    width = own // n_rhs
    share = pl.ds(pl.multiple_of(x * width, width), width)
    shared = pts_late.at[:, share]
    quarter = remote(points.at[:, share], shared, halo_send.at[7], halo_recv.at[7], outside)
    copies = [
        remote(shared, shared, share_send.at[d], share_recv.at[d], peer)
        for d, peer in x_peers.items()
    ]
    pl.when(stays)(halves[0].start)
    pl.when(crosses)(quarter.start)
    with jax.named_scope("lists"):
        for copy in list_loads:
            copy.wait()
        next_early[entries] = entries
        next_late[entries] = entries
        source_of[entries] = 0

        def link(i, carry):
            following, following_late = carry
            l = leaves - 1 - i
            count = near_count[l]
            for s in range(per_leaf, 0, -1):
                e = l * per_leaf + s - 1
                segment, inner = place(near_list[s, l], me, core, devices, leaves)
                used = s < count
                following = jnp.where(used & (segment < 2), e, following)
                following_late = jnp.where(used & (segment == 2), e, following_late)
                next_early[e] = following
                next_late[e] = following_late
                source_of[e] = segment * leaves + inner
            return following, following_late

        lax.fori_loop(0, leaves, link, (i32(entries), i32(entries)))

        def number(l, carry):
            count, count_late = carry
            for s in range(per_leaf):
                e = l * per_leaf + s
                is_early = next_early[e] == e
                is_late = next_late[e] == e
                slot = jnp.where(is_early & (count < EARLY), count, EARLY + LATE)
                slot = jnp.where(is_late & (count_late < LATE), EARLY + count_late, slot)
                slot_of[e] = slot
                count = count + jnp.where(is_early, 1, 0)
                count_late = count_late + jnp.where(is_late, 1, 0)
            return count, count_late

        count, count_late = lax.fori_loop(0, leaves, number, (i32(0), i32(0)))
        over[0] = jnp.maximum(count - EARLY, 0) + jnp.maximum(count_late - LATE, 0)
        slots[EARLY + LATE] = jnp.zeros_like(slots[EARLY + LATE])

    with jax.named_scope("selfs"):
        points_load.wait()

        def build(g, carry):
            for member in range(2):
                l = g * 2 + member
                targets[l] = as_target(pts[:, pl.ds(pl.multiple_of(l * leaf, leaf), leaf)])
            return carry

        lax.fori_loop(0, leaves // 2, build, 0)

        def prepare(points_from, vectors_from, start, base):
            def turn(g, carry):
                for member in range(2):
                    l = g * 2 + member
                    there = pl.ds(pl.multiple_of(start * leaf + l * leaf, leaf), leaf)
                    sources[base + l] = as_source(points_from[:, there])
                    values[base + l] = vectors_from[:, there]
                return carry

            lax.fori_loop(0, leaves // 2, turn, 0)

        prepare(pts, vec, 0, 0)

    def self_turn(g, carry):
        for member in range(GROUP):
            l = g * GROUP + member
            near[l] = pair(features, targets[l], sources[l], values[l])
        return carry

    with jax.named_scope("self1"):
        lax.fori_loop(0, 2, self_turn, 0)
    pl.when(stays)(halves[1].start)
    late_vectors = send_halo(5, vectors, vec_late, outside)
    with jax.named_scope("relay"):
        lines[last - 1].wait_recv()
        pl.when(core == 0)(relay.start)
    with jax.named_scope("forward1"):
        pl.when(core == 0)(lines[0].wait_recv)
        for k in range(1, last - 1):
            lines[k].wait_recv()
        pl.when(core == 0)(lambda: forward(0))
        for k in range(1, last):
            forward(k)
    with jax.named_scope("self2"):
        lax.fori_loop(2, leaves // GROUP, self_turn, 0)
    with jax.named_scope("quarter"):

        @pl.when(crosses)
        def _():
            quarter.wait_recv()
            for copy in copies:
                copy.start()

        moments.append(send_halo(6, own_moments, mom.at[pl.ds(2 * leaves, leaves)], outside))

    def list_turns(turns, base, following, start):
        def turn(g, e):
            for member in range(GROUP):
                l = jnp.minimum(e // per_leaf, leaves - 1)
                there = source_of[e]
                slots[base + g * GROUP + member] = pair(
                    features, targets[l], sources[there], values[there]
                )
                e = following[jnp.minimum(e + 1, entries)]
            return e

        return lax.fori_loop(0, turns, turn, start)

    with jax.named_scope("early"):
        for copy in early:
            copy.wait_recv()
        prepare(pts, vec, leaves, leaves)
        at = list_turns(2, 0, next_early, next_early[0])
    with jax.named_scope("forward2"):
        lines[last].wait_recv()
        forward(last)
        lifted_pair = send(line.at[:, 1], lifted, pair_send.at[1], pair_recv.at[1], partner)
    with jax.named_scope("early2"):
        list_turns(EARLY // GROUP - 2, 2 * GROUP, next_early, at)
    with jax.named_scope("top_part"):
        for copy in coupling_loads:
            copy.wait()
        lifted_pair.wait_recv()
        top_part = None
        for k in range(half):
            below, above = (z + n_z - k - 1) % n_z, (z + k) % n_z
            near_z = jnp.where(core == 0, below, above)
            other_z = jnp.where(core == 0, above, below)
            for c in range(2):
                part = dot(line[k, 1, c], tcp[0, 2 * near_z + c])
                top_part = part if top_part is None else top_part + part
                top_part = top_part + dot(lifted[k, c], tcp[0, 2 * other_z + c])
        top_parts[row] = top_part
        top_sends = [
            send(top_parts.at[row], top_parts.at[row], top_send.at[q], top_recv.at[q], y_peer(q))
            for q in y_steps
        ]
    saves = [
        load(15, pts.at[:, pl.ds(own, own)], halo_points.at[0]),
        load(16, vec.at[:, pl.ds(own, own)], halo_vectors.at[0]),
    ]
    with jax.named_scope("late_wait"):
        late_vectors.wait_recv()

        @pl.when(stays)
        def _():
            for copy in halves:
                copy.wait_recv()

        @pl.when(crosses)
        def _():
            for copy in copies:
                copy.wait_recv()

        prepare(pts_late, vec_late, 0, 2 * leaves)
    saves += [load(17, pts_late, halo_points.at[1]), load(18, vec_late, halo_vectors.at[1])]
    with jax.named_scope("late"):
        at = list_turns(2, EARLY, next_late, next_late[0])
    gives = []
    with jax.named_scope("give"):
        for k in range(half):
            for q in y_steps:
                far[k, q].wait_recv()
            ref = nodes.at[core, k]
            gives.append(send(ref, ref, give_send.at[k], give_recv.at[k], partner))
    with jax.named_scope("late2"):
        list_turns(LATE // GROUP - 2, EARLY + 2 * GROUP, next_late, at)
        for copy in moments:
            copy.wait_recv()
    with jax.named_scope("gather"):

        def gather(l, carry):
            total = near[l]
            for s in range(per_leaf):
                total = total + slots[slot_of[l * per_leaf + s]]
            near[l] = total
            return carry

        lax.fori_loop(0, leaves, gather, 0)
    fields = []
    for l in range(leaves):
        total = None
        for k in range(far_leaves.shape[0]):
            segment, inner = place(far_leaves[k, l], me, core, devices, leaves)
            part = dot(mom[segment * leaves + inner], lcp[l, k])
            total = part if total is None else total + part
        fields.append(total)
    with jax.named_scope("gives_wait"):
        for copy in top_sends:
            copy.wait_recv()
        for copy in gives:
            copy.wait_recv()

    with jax.named_scope("tail"):
        node_field = None
        for k in range(far_nodes.shape[1]):
            m = far_nodes[0, k]
            step = ((m % n_col) // 2 + n_z - z) % n_z
            side = jnp.where(step < half, 1, 0)
            place_at = jnp.where(step < half, step, n_z - 1 - step)
            part = dot(nodes[side, place_at, m // n_col, m % 2], ncp[0, k])
            node_field = part if node_field is None else node_field + part
        top_field = top_parts[0]
        for r in range(1, n_row):
            top_field = top_field + top_parts[r]
        node_down = (node_field + dot_nt(top_field.astype(bf16), ntr[0])).astype(bf16)
        for l in range(leaves):
            down = (fields[l] + dot_nt(node_down, ltr[l])).astype(bf16)
            result[l] = near[l] + dot_nt(down, bas[l])
            if (l + 1) % chunk == 0:
                done = pl.ds(l + 1 - chunk, chunk)
                saves.append(load(19 + l // chunk, result.at[done], partial.at[done]))
    with jax.named_scope("ends"):
        for copy in saves:
            copy.wait()
        for copy in started:
            copy.wait_send()
        for copy in far.values():
            copy.wait_send()
        pl.when(core == 0)(lines[0].wait_send)

        @pl.when(stays)
        def _():
            for copy in halves:
                copy.wait_send()

        @pl.when(crosses)
        def _():
            for copy in [quarter] + copies:
                copy.wait_send()

        for k in range(1, half):
            lines[k].wait_send()


def rest_kernel(
    n_row,
    n_col,
    over,
    near_list_in,
    near_count_in,
    points,
    vectors,
    halo_points,
    halo_vectors,
    partial,
    product,
    near_list,
    near_count,
    total,
    rounded,
    own_points,
    there_points,
    there_vectors,
    sem,
    chunk_sem,
):
    col = lax.axis_index("col")
    me = lax.axis_index("row") * n_col + col
    core = col % 2
    leaves, columns, leaf = total.shape
    per_leaf = near_list.shape[0] - 1
    chunk = leaves // 4
    loads = []
    for c in range(4):
        part = pl.ds(c * chunk, chunk)
        loads.append(pltpu.make_async_copy(partial.at[part], total.at[part], chunk_sem.at[c]))
        loads[c].start()

    def store(c):
        span = pl.ds(c * chunk * leaf, chunk * leaf)
        return pltpu.make_async_copy(
            rounded.at[:, span], product.at[:, span], chunk_sem.at[4 + c]
        )

    def finish(c):
        for l in range(c * chunk, (c + 1) * chunk):
            rounded[:, l * leaf : (l + 1) * leaf] = total[l].astype(bf16)
        store(c).start()

    @pl.when(over[0] == 0)
    def _():
        for c in range(4):
            loads[c].wait()
            finish(c)

    @pl.when(over[0] > 0)
    def _():
        lists = [
            pltpu.make_async_copy(near_list_in, near_list, sem.at[0]),
            pltpu.make_async_copy(near_count_in, near_count, sem.at[1]),
        ]
        for copy in lists:
            copy.start()
        for copy in lists + loads:
            copy.wait()
        def entry(e, carry):
            count, count_late = carry
            l = e // per_leaf
            s = e % per_leaf + 1
            segment, inner = place(near_list[s, l], me, core, n_row * n_col, leaves)
            used = s < near_count[l]
            is_early, is_late = used & (segment < 2), used & (segment == 2)
            missed = (is_early & (count >= EARLY)) | (is_late & (count_late >= LATE))

            def fetch(slot, src, dst):
                copy = pltpu.make_async_copy(src, dst, sem.at[slot])
                copy.start()
                copy.wait()

            @pl.when(missed)
            def _():
                here = pl.ds(pl.multiple_of(l * leaf, leaf), leaf)
                there = pl.ds(pl.multiple_of(inner * leaf, leaf), leaf)
                fetch(0, points.at[:, here], own_points)

                @pl.when(segment == 0)
                def _():
                    fetch(1, points.at[:, there], there_points)
                    fetch(2, vectors.at[:, there], there_vectors)

                @pl.when(segment > 0)
                def _():
                    fetch(1, halo_points.at[segment - 1, :, there], there_points)
                    fetch(2, halo_vectors.at[segment - 1, :, there], there_vectors)

                target, source = as_target(own_points[...]), as_source(there_points[...])
                total[l] += pair(own_points.shape[0], target, source, there_vectors[...])

            return count + jnp.where(is_early, 1, 0), count_late + jnp.where(is_late, 1, 0)

        lax.fori_loop(0, leaves * per_leaf, entry, (i32(0), i32(0)))
        for c in range(4):
            finish(c)

    for c in range(4):
        store(c).wait()


def whole(n_row, n_col, n_rhs, *arrays):
    points, vectors, basis, transfer, node_transfer = arrays[:5]
    leaf_coupling, node_coupling, top_coupling, near_list, near_count, far_leaves, far_nodes = arrays[5:12]
    leaves, leaf, rank = basis.shape
    features, columns = points.shape[0], vectors.shape[0]
    own = leaves * leaf
    half = n_col // 4
    entries = leaves * (near_list.shape[0] - 1)
    anywhere = pl.BlockSpec(memory_space=pl.ANY)
    smem = pl.BlockSpec(memory_space=pltpu.SMEM)
    dma = pltpu.SemaphoreType.DMA
    partial, halo_points, halo_vectors, over = pl.pallas_call(
        functools.partial(kernel, n_row, n_col, n_rhs),
        out_shape=(
            jax.ShapeDtypeStruct((leaves, columns, leaf), f32),
            jax.ShapeDtypeStruct((2, features, own), bf16),
            jax.ShapeDtypeStruct((2, columns, own), bf16),
            jax.ShapeDtypeStruct((1,), i32),
        ),
        in_specs=[anywhere] * 12,
        out_specs=(anywhere, anywhere, anywhere, smem),
        scratch_shapes=[
            pltpu.VMEM((leaves, columns, leaf), f32),
            pltpu.SMEM(near_list.shape, i32),
            pltpu.SMEM(near_count.shape, i32),
            pltpu.SMEM(far_leaves.shape, i32),
            pltpu.SMEM(far_nodes.shape, i32),
            pltpu.VMEM((features, 2 * own), bf16),
            pltpu.VMEM((features, own), bf16),
            pltpu.VMEM((columns, 2 * own), bf16),
            pltpu.VMEM((columns, own), bf16),
            pltpu.VMEM((leaves, leaf, 128), bf16),
            pltpu.VMEM((3 * leaves, 128, leaf), bf16),
            pltpu.VMEM((3 * leaves, columns, leaf), bf16),
            pltpu.VMEM((leaves, columns, leaf), f32),
            pltpu.VMEM((EARLY + LATE + 1, columns, leaf), f32),
            pltpu.VMEM((3 * leaves, columns, rank), bf16),
            pltpu.VMEM((2, 2, columns, rank), bf16),
            pltpu.VMEM((half, 2, 2, columns, rank), bf16),
            pltpu.VMEM((2, half, n_row, 2, columns, rank), bf16),
            pltpu.VMEM((half, 2, columns, rank), bf16),
            pltpu.VMEM((n_row, columns, rank), f32),
            pltpu.VMEM(basis.shape, bf16),
            pltpu.VMEM(transfer.shape, bf16),
            pltpu.VMEM(node_transfer.shape, bf16),
            pltpu.VMEM(leaf_coupling.shape, bf16),
            pltpu.VMEM(node_coupling.shape, bf16),
            pltpu.VMEM(top_coupling.shape, bf16),
            pltpu.SMEM((entries + 1,), i32),
            pltpu.SMEM((entries + 1,), i32),
            pltpu.SMEM((entries + 1,), i32),
            pltpu.SMEM((entries,), i32),
            dma((23,)),
            dma((2,)),
            dma((2,)),
            dma((n_row,)),
            dma((n_row,)),
            dma((half,)),
            dma((half,)),
            dma((half, n_row)),
            dma((half, n_row)),
            dma((half,)),
            dma((half,)),
            dma((8,)),
            dma((8,)),
            dma((n_rhs,)),
            dma((n_rhs,)),
        ],
        compiler_params=pltpu.CompilerParams(collective_id=0, has_side_effects=True),
        name="hierarchy",
    )(*arrays)
    return pl.pallas_call(
        functools.partial(rest_kernel, n_row, n_col),
        out_shape=jax.ShapeDtypeStruct(vectors.shape, bf16),
        in_specs=[smem] + [anywhere] * 7,
        out_specs=anywhere,
        scratch_shapes=[
            pltpu.SMEM(near_list.shape, i32),
            pltpu.SMEM(near_count.shape, i32),
            pltpu.VMEM((leaves, columns, leaf), f32),
            pltpu.VMEM(vectors.shape, bf16),
            pltpu.VMEM((features, leaf), bf16),
            pltpu.VMEM((features, leaf), bf16),
            pltpu.VMEM((columns, leaf), bf16),
            dma((3,)),
            dma((8,)),
        ],
        name="rest",
    )(over, near_list, near_count, points, vectors, halo_points, halo_vectors, partial)


def solution(mesh):
    n_row, n_col, n_rhs = mesh.shape["row"], mesh.shape["col"], mesh.shape["rhs"]

    def local(
        points,
        vectors,
        leaf_basis,
        leaf_transfer,
        node_transfer,
        leaf_coupling,
        node_coupling,
        top_coupling,
        near_list,
        near_count,
        far_leaves,
        far_nodes,
    ):
        return whole(
            n_row,
            n_col,
            n_rhs,
            points,
            vectors,
            leaf_basis,
            leaf_transfer,
            node_transfer,
            leaf_coupling,
            node_coupling,
            top_coupling,
            near_list.T,
            near_count,
            far_leaves.T,
            far_nodes,
        )

    return jax.shard_map(
        local,
        mesh=mesh,
        in_specs=(
            P(None, ("row", "col")),
            P("rhs", ("row", "col")),
            P(("row", "col"), None, None),
            P(("row", "col"), None, None),
            P(("row", "col"), None, None),
            P(("row", "col"), None, None, None),
            P(("row", "col"), None, None, None),
            P("col", None, None, None),
            P(("row", "col"), None),
            P(("row", "col")),
            P(("row", "col"), None),
            P(("row", "col"), None),
        ),
        out_specs=P("rhs", ("row", "col")),
        check_vma=False,
    )
```
